512 devices in a mesh: batch: 8 (over y_lo, x), rows: 8 (over z), chan: 8 (over y_hi, core).
Axes of the slice: x: 4, y: 8 (y_hi: 4, y_lo: 2; y = y_hi * 2 + y_lo), z: 8, core: 2. Of those that a mesh axis runs over, the one named last changes fastest.
Arguments:
- images: float32 [64, 24, 64, 32], P('batch', None, ('rows', 'chan')), may hold values from -6 to 6
- shift_mid: float32 [3, 24], replicated, may hold values from -1.75 to 1.75
- gain_mid: float32 [3, 24], replicated, may hold values from -0.3 to 0.3
- lower_mid: float32 [3, 24, 24], replicated, may hold values from -1.25 to 1.25
- upper_mid: float32 [3, 24, 24], replicated, may hold values from -1.25 to 1.25
- diag_mid: float32 [3, 24], replicated, may hold values from -0.3 to 0.3
- first_mid: bfloat16 [3, 9, 12, 512], replicated, may hold values from -0.625 to 0.625
- first_bias_mid: bfloat16 [3, 512], replicated, may hold values from -3 to 3
- second_mid: bfloat16 [3, 512, 512], replicated, may hold values from -0.25 to 0.25
- second_bias_mid: float32 [3, 512], replicated, may hold values from -3 to 3
- third_mid: bfloat16 [3, 9, 512, 24], replicated, may hold values from -0.09375 to 0.09375
- third_bias_mid: float32 [3, 24], replicated, may hold values from -3 to 3
- shift_top: float32 [2, 48], replicated, may hold values from -1.75 to 1.75
- gain_top: float32 [2, 48], replicated, may hold values from -0.3 to 0.3
- lower_top: float32 [2, 48, 48], replicated, may hold values from -0.875 to 0.875
- upper_top: float32 [2, 48, 48], replicated, may hold values from -0.875 to 0.875
- diag_top: float32 [2, 48], replicated, may hold values from -0.3 to 0.3
- first_top: bfloat16 [2, 9, 24, 512], replicated, may hold values from -0.4375 to 0.4375
- first_bias_top: bfloat16 [2, 512], replicated, may hold values from -3 to 3
- second_top: bfloat16 [2, 512, 512], replicated, may hold values from -0.25 to 0.25
- second_bias_top: float32 [2, 512], replicated, may hold values from -3 to 3
- third_top: bfloat16 [2, 9, 512, 48], replicated, may hold values from -0.09375 to 0.09375
- third_bias_top: float32 [2, 48], replicated, may hold values from -3 to 3
Outputs:
- latent_mid: float32 [64, 12, 64, 32], P('batch', None, ('rows', 'chan'))
- latent_top: float32 [64, 48, 32, 16], P(('batch', 'chan'), None, 'rows')
- loglik: float32 [64], P(('batch', 'chan'))
The draws below stay inside these ranges and needn't reach their ends.
All inputs are finite; a program needn't handle non-finite values.
Results may differ from the reference program's by a relative error of at most 0.008.
Values may be sent and summed in bfloat16 or wider, within the bound.
A program may use at most 64 MiB of HBM per device.

```python
import math
import jax
import jax.numpy as jnp
from jax import lax

HID = 512
C2 = 24
W2 = 32
STEPS2 = 3
STEPS3 = 2
B = 64
H2 = 64
C3 = 48


def level_of(rng, extent, split, least, high):
    gain, own = 1.0, jax.random.fold_in(rng, 6)
    for axis_at, shards_of in split:
        draws = jnp.exp(jax.random.uniform(jax.random.fold_in(own, axis_at), (shards_of,), jnp.float32, least / len(split), high / len(split)))
        gain = gain * jnp.repeat(draws, extent[axis_at] // shards_of).reshape([-1 if axis == axis_at else 1 for axis in range(len(extent))])
    return gain


def centred(rng, dims, width, bound, shards=(), held_as=jnp.bfloat16):
    array = width * jax.random.normal(rng, dims, jnp.float32)
    if shards:
        array = array * level_of(rng, dims, shards, -0.22, 0.18)
    return jnp.clip(array, -bound, bound).astype(held_as)


def setup_inputs(seed: int = 0) -> dict:
    keys = jax.random.split(jax.random.key(seed), 24)
    return {
        "images": centred(keys[0], (B, C2, H2, W2), 1.0, 6.0, ((0, 8), (2, 64)), jnp.float32),
        "shift_mid": centred(keys[1], (STEPS2, C2), 0.3, 1.75, (), jnp.float32),
        "gain_mid": jnp.clip(jax.random.uniform(keys[2], (STEPS2, C2), jnp.float32, -0.3, 0.3), -0.3, 0.3),
        "lower_mid": centred(keys[3], (STEPS2, C2, C2), C2 ** -0.5, 1.25, (), jnp.float32),
        "upper_mid": centred(keys[4], (STEPS2, C2, C2), C2 ** -0.5, 1.25, (), jnp.float32),
        "diag_mid": jnp.clip(jax.random.uniform(keys[5], (STEPS2, C2), jnp.float32, -0.3, 0.3), -0.3, 0.3),
        "first_mid": centred(keys[6], (STEPS2, 9, C2 // 2, HID), (9 * C2 // 2) ** -0.5, 0.625),
        "first_bias_mid": centred(keys[7], (STEPS2, HID), 0.5, 3.0),
        "second_mid": centred(keys[8], (STEPS2, HID, HID), HID ** -0.5, 0.25),
        "second_bias_mid": centred(keys[9], (STEPS2, HID), 0.5, 3.0, (), jnp.float32),
        "third_mid": centred(keys[10], (STEPS2, 9, HID, C2), (9 * HID) ** -0.5, 0.09375),
        "third_bias_mid": centred(keys[11], (STEPS2, C2), 0.5, 3.0, (), jnp.float32),
        "shift_top": centred(keys[12], (STEPS3, C3), 0.3, 1.75, (), jnp.float32),
        "gain_top": jnp.clip(jax.random.uniform(keys[13], (STEPS3, C3), jnp.float32, -0.3, 0.3), -0.3, 0.3),
        "lower_top": centred(keys[14], (STEPS3, C3, C3), C3 ** -0.5, 0.875, (), jnp.float32),
        "upper_top": centred(keys[15], (STEPS3, C3, C3), C3 ** -0.5, 0.875, (), jnp.float32),
        "diag_top": jnp.clip(jax.random.uniform(keys[16], (STEPS3, C3), jnp.float32, -0.3, 0.3), -0.3, 0.3),
        "first_top": centred(keys[17], (STEPS3, 9, C2, HID), (9 * C2) ** -0.5, 0.4375),
        "first_bias_top": centred(keys[18], (STEPS3, HID), 0.5, 3.0),
        "second_top": centred(keys[19], (STEPS3, HID, HID), HID ** -0.5, 0.25),
        "second_bias_top": centred(keys[20], (STEPS3, HID), 0.5, 3.0, (), jnp.float32),
        "third_top": centred(keys[21], (STEPS3, 9, HID, C3), (9 * HID) ** -0.5, 0.09375),
        "third_bias_top": centred(keys[22], (STEPS3, C3), 0.5, 3.0, (), jnp.float32),
    }


log_two_pi = math.log(2.0 * math.pi)


def spatial_conv(source, weights):
    height = source.shape[1]
    columns = source.shape[2]
    padded = jnp.pad(source, ((0, 0), (1, 1), (1, 1))).astype(jnp.float32)
    summed = jnp.zeros((weights.shape[2], height, columns), jnp.float32)
    for tap_idx in range(9):
        row_off = tap_idx // 3
        col_off = tap_idx % 3
        window = padded[:, row_off:row_off + height, col_off:col_off + columns]
        summed = summed + jnp.einsum('chw,co->ohw', window, weights[tap_idx].astype(jnp.float32))
    return summed


def flow_step(flow_state, params):
    shift_vec, gain_vec, lower_raw, upper_raw, diag_log, first_w, first_b, second_w, second_b, third_w, third_b = params
    channels = flow_state.shape[0]
    half_chan = channels // 2
    cell_count = flow_state.shape[1] * flow_state.shape[2]
    mixed_state = (flow_state + shift_vec[:, None, None]) * jnp.exp(gain_vec)[:, None, None]
    lower_mat = jnp.tril(lower_raw, -1) + jnp.eye(channels, dtype=jnp.float32)
    upper_mat = jnp.triu(upper_raw, 1) + jnp.diag(jnp.exp(diag_log))
    matrix = jnp.dot(lower_mat, upper_mat, precision=lax.Precision.HIGHEST)
    mixed_state = jnp.einsum('oc,chw->ohw', matrix, mixed_state, precision=lax.Precision.HIGHEST)
    part_a = mixed_state[:half_chan]
    part_b = mixed_state[half_chan:]
    coupled = part_a.astype(jnp.bfloat16)
    inner = jax.nn.relu(spatial_conv(coupled, first_w) + first_b.astype(jnp.float32)[:, None, None]).astype(jnp.bfloat16)
    middle = jnp.einsum('chw,co->ohw', inner.astype(jnp.float32), second_w.astype(jnp.float32))
    middle = jax.nn.relu(middle + second_b[:, None, None]).astype(jnp.bfloat16)
    output = spatial_conv(middle, third_w) + third_b[:, None, None]
    gate_pre = output[:half_chan] + 2.0
    updated = (part_b + output[half_chan:]) * jax.nn.sigmoid(gate_pre)
    step_term = cell_count * (jnp.sum(gain_vec) + jnp.sum(diag_log)) + jnp.sum(jax.nn.log_sigmoid(gate_pre))
    return jnp.concatenate([part_a, updated], axis=0), step_term


def image_flow(picture, params_mid, params_top):
    flow_state = picture
    logdet = jnp.zeros((), jnp.float32)
    for step_num in range(params_mid[0].shape[0]):
        flow_state, step_term = flow_step(flow_state, tuple(p[step_num] for p in params_mid))
        logdet = logdet + step_term
    half_chan = flow_state.shape[0] // 2
    latent_mid = flow_state[:half_chan]
    kept_chan = flow_state[half_chan:]
    count_chan, height, columns = kept_chan.shape
    squeezed = kept_chan.reshape(count_chan, height // 2, 2, columns // 2, 2).transpose(0, 2, 4, 1, 3)
    flow_state = squeezed.reshape(count_chan * 4, height // 2, columns // 2)
    for step_num in range(params_top[0].shape[0]):
        flow_state, step_term = flow_step(flow_state, tuple(p[step_num] for p in params_top))
        logdet = logdet + step_term
    latent_top = flow_state
    latent_count = latent_mid.size + latent_top.size
    logprob = -0.5 * (jnp.sum(latent_mid * latent_mid) + jnp.sum(latent_top * latent_top)) - 0.5 * log_two_pi * latent_count
    total_dims = picture.shape[0] * picture.shape[1] * picture.shape[2]
    return latent_mid, latent_top, (logprob + logdet) / total_dims


def reference(images, shift_mid, gain_mid, lower_mid, upper_mid, diag_mid, first_mid, first_bias_mid, second_mid, second_bias_mid, third_mid, third_bias_mid, shift_top, gain_top, lower_top, upper_top, diag_top, first_top, first_bias_top, second_top, second_bias_top, third_top, third_bias_top):
    params_mid = (shift_mid, gain_mid, lower_mid, upper_mid, diag_mid, first_mid, first_bias_mid, second_mid, second_bias_mid, third_mid, third_bias_mid)
    params_top = (shift_top, gain_top, lower_top, upper_top, diag_top, first_top, first_bias_top, second_top, second_bias_top, third_top, third_bias_top)
    latent_mid, latent_top, loglik = lax.map(lambda picture: image_flow(picture, params_mid, params_top), images)
    return (latent_mid, latent_top, loglik)
```

```python
import math

import jax
import jax.numpy as jnp
from jax import lax
from jax.experimental import pallas as pl
from jax.experimental.pallas import tpu as pltpu
from jax.sharding import PartitionSpec as P

MESH = pl.DeviceIdType.MESH
F32 = jnp.float32
BF16 = jnp.bfloat16
LOG_TWO_PI = math.log(2.0 * math.pi)

HID = 512
ROWS = 8
CHAN = 8
C2, C3 = 24, 48
STEPS2, STEPS3 = 3, 2
COLS = 32
LANES = 128
REACH = 2
BLOCKS = 2 * REACH + 1
WIDE = BLOCKS * 8 * COLS
NARROW = WIDE - 2 * LANES
KMID = 160
KTOP = 224
NTOP = 256
DIMS = 24 * 64 * 32


def iota(shape, dim):
    return lax.broadcasted_iota(jnp.int32, shape, dim)


def dot(a, b):
    return jnp.dot(a, b, preferred_element_type=F32)


def exact_dot(a, b):
    return jnp.dot(a, b, preferred_element_type=F32, precision=lax.Precision.HIGHEST)


def column(row):
    n = row.shape[1]
    eye = iota((n, n), 0) == iota((n, n), 1)
    return jnp.sum(jnp.where(eye, row, 0.0), axis=1, keepdims=True)


def place_mid(n, dim):
    at = iota((n, n), dim)
    return jnp.where(at < 12, at, jnp.where(at < 16, at + 8, at - 4))


def mixing(shift, gain, lower, upper, diag):
    n = shift.shape[1]
    i, j = iota((n, n), 0), iota((n, n), 1)
    low = jnp.where(j < i, lower, 0.0) + jnp.where(i == j, 1.0, 0.0)
    up = jnp.where(j > i, upper, 0.0) + jnp.where(i == j, jnp.exp(diag), 0.0)
    a = exact_dot(low, up) * jnp.exp(gain)
    return a, jnp.sum(a * shift, axis=1, keepdims=True)


def stacked(a, b, width, bias_at):
    rows, n = a.shape
    if width > n:
        a = jnp.concatenate([a, jnp.zeros((rows, width - n), F32)], axis=1)
    a = jnp.where(iota((rows, width), 1) == bias_at, b, a)
    high = a.astype(BF16).astype(F32)
    low = a - high
    return jnp.concatenate([high, high, low], axis=1).astype(BF16)


def split_mix(a, v):
    high = v.astype(BF16)
    low = (v - high.astype(F32)).astype(BF16)
    return dot(a, jnp.concatenate([high, low, high], axis=0))


def roll(x, by):
    n = x.shape[1]
    by = by % n
    return x if by == 0 else pltpu.roll(x, by, 1)


def ones_block(n, height, at):
    return jnp.where(iota((height, n), 0) == at, 1.0, 0.0)


def conditioner(q, inside, width, w1, w2, b2, w3, b3):
    n = q.shape[1]
    col = iota((1, n), 1) % width
    from_left, from_right = col > 0, col < width - 1
    left = jnp.where(from_left, roll(q, 1), 0.0)
    right = jnp.where(from_right, roll(q, -1), 0.0)
    taps = [roll(side, -width * dy) for dy in (-1, 0, 1) for side in (left, q, right)]
    taps.append(ones_block(n, w1.shape[1] - 9 * q.shape[0], 0))
    patches = jnp.concatenate(taps, axis=0).astype(BF16)
    pieces = []
    for at in range(0, n, 256):
        h1 = jnp.maximum(dot(w1[...], patches[:, at : at + 256]), 0.0).astype(BF16)
        bias = jnp.concatenate([b2[...]] * 2, axis=1)
        h2 = jnp.maximum(dot(w2[...], h1) + bias, 0.0).astype(BF16)
        pieces.append(dot(w3[...], h2))
    z = pieces[0] if len(pieces) == 1 else jnp.concatenate(pieces, axis=1)
    z = jnp.where(inside, z, 0.0)
    outs = w3.shape[0] // 9
    sides = []
    for dx in range(3):
        total = z[(3 + dx) * outs : (4 + dx) * outs]
        total += roll(z[dx * outs : (dx + 1) * outs], width)
        total += roll(z[(6 + dx) * outs : (7 + dx) * outs], -width)
        sides.append(total)
    out = sides[1] + jnp.where(from_left, roll(sides[0], 1), 0.0)
    out += jnp.where(from_right, roll(sides[2], -1), 0.0)
    return out + b3


def gate(g):
    small = jnp.exp(-jnp.abs(g))
    sigmoid = jnp.where(g >= 0.0, 1.0, small) / (1.0 + small)
    return sigmoid, jnp.minimum(g, 0.0) - jnp.log(1.0 + small)


def kernel(
    images,
    shift_mid,
    gain_mid,
    lower_mid,
    upper_mid,
    diag_mid,
    first_mid,
    first_bias_mid,
    second_mid,
    second_bias_mid,
    third_mid,
    third_bias_mid,
    shift_top,
    gain_top,
    lower_top,
    upper_top,
    diag_top,
    first_top,
    first_bias_top,
    second_top,
    second_bias_top,
    third_top,
    third_bias_top,
    latent_mid,
    latent_top,
    loglik,
    pictures,
    packed,
    arrived,
    first2,
    second2,
    third2,
    first3,
    second3,
    third3,
    small2,
    small3,
    mix2,
    mix3,
    bias2,
    bias3,
    tall,
    w1_mid,
    w2_mid,
    b2_mid,
    w3_mid,
    w1_top,
    w2_top,
    b2_top,
    w3_top,
    sent_latent,
    got_latent,
    terms,
    load_sem,
    small_sem,
    weight_sem,
    send_sem,
    recv_sem,
    latent_send,
    latent_recv,
    term_send,
    term_recv,
):
    r, c = lax.axis_index("rows"), lax.axis_index("chan")
    barrier = pltpu.get_barrier_semaphore()

    picture_load = pltpu.make_async_copy(images, pictures, load_sem)
    picture_load.start()
    given2 = (shift_mid, gain_mid, lower_mid, upper_mid, diag_mid, first_bias_mid, second_bias_mid, third_bias_mid)
    given3 = (shift_top, gain_top, lower_top, upper_top, diag_top, first_bias_top, second_bias_top, third_bias_top)
    small_loads = [
        pltpu.make_async_copy(src, dst, small_sem.at[i])
        for i, (src, dst) in enumerate(zip(given2 + given3, small2 + small3))
    ]
    for load in small_loads:
        load.start()
    weight_loads = []
    for s in range(STEPS2):
        for src, dst in ((second_mid, second2), (first_mid, first2), (third_mid, third2)):
            weight_loads.append(
                pltpu.make_async_copy(src.at[s], dst.at[s], weight_sem.at[len(weight_loads)])
            )
    for s in range(STEPS3):
        for src, dst in ((second_top, second3), (first_top, first3), (third_top, third3)):
            weight_loads.append(
                pltpu.make_async_copy(src.at[s], dst.at[s], weight_sem.at[len(weight_loads)])
            )
    for load in weight_loads:
        load.start()

    def in_image(d, body):
        if d == 0:
            body()
        else:
            pl.when((r + d >= 0) & (r + d < ROWS))(body)

    near = range(-REACH, REACH + 1)

    arrived[...] = jnp.zeros_like(arrived)
    for d in near:

        def greet(d=d):
            for k in range(1 if d == 0 else 0, CHAN):
                pl.semaphore_signal(
                    barrier, 1, device_id={"rows": r + d, "chan": (c + k) % CHAN}, device_id_type=MESH
                )

        in_image(d, greet)
    for d in range(REACH + 1, ROWS):
        for far in (-d, d):

            def greet_far(far=far):
                pl.semaphore_signal(barrier, 1, device_id={"rows": r + far}, device_id_type=MESH)

            in_image(far, greet_far)

    picture_load.wait()
    group = iota((8, LANES), 1) // COLS
    for i in range(8):
        tile = jnp.zeros((8, LANES), F32)
        for k in range(3):
            part = pictures[i, 8 * k : 8 * k + 8, :]
            part = jnp.concatenate([part, jnp.zeros((8, LANES - COLS), F32)], axis=1)
            tile = jnp.where(group == k, roll(part, COLS * k), tile)
        packed[i] = tile

    def prepare_small():
        for load in small_loads:
            load.wait()
        shift, gain, lower, upper, diag, _, second_b, third_b = small2
        for s in range(STEPS2):
            a, b = mixing(shift[s : s + 1], gain[s : s + 1], lower[s], upper[s], diag[s : s + 1])
            to_rows = jnp.where(place_mid(C2, 0) == iota((C2, C2), 1), 1.0, 0.0)
            a = exact_dot(to_rows, a)
            if s:
                to_columns = jnp.where(place_mid(C2, 1) == iota((C2, C2), 0), 1.0, 0.0)
                a = exact_dot(a, to_columns)
            b = exact_dot(to_rows, b)
            mix2[s] = stacked(a, b, 32, C2)
            extra = third_b[s : s + 1] + jnp.where(iota((1, C2), 1) < C2 // 2, 2.0, 0.0)
            bias2[s] = jnp.sum(to_rows * extra, axis=1, keepdims=True)
            b2_mid[s] = jnp.broadcast_to(second_b[s : s + 1], (LANES, HID)).T
        shift, gain, lower, upper, diag, _, second_b, third_b = small3
        for s in range(STEPS3):
            a, b = mixing(shift[s : s + 1], gain[s : s + 1], lower[s], upper[s], diag[s : s + 1])
            if s == 0:
                n, k = iota((C3, 64), 0), iota((C3, 64), 1)
                row = n // 4
                at = (n % 4) * 16 + jnp.where(row < 8, row, row + 4)
                a = exact_dot(a, jnp.where(at == k, 1.0, 0.0))
                mix3[s] = stacked(a, b, 80, 64)
            else:
                mix3[s] = stacked(a, b, 80, C3)
            extra = third_b[s : s + 1] + jnp.where(iota((1, C3), 1) < C3 // 2, 2.0, 0.0)
            bias3[s] = column(extra)
            b2_top[s] = jnp.broadcast_to(second_b[s : s + 1], (LANES, HID)).T

    def prepare_mid(s):
        for i in range(3):
            weight_loads[3 * s + i].wait()
        w2_mid[s] = second2[s].T
        tall[...] = jnp.zeros_like(tall)
        for t in range(9):
            tall[16 * t : 16 * t + 12, :] = first2[s, t].astype(F32)
        tall[144:145, :] = small2[5][s : s + 1].astype(F32)
        w1_mid[s] = tall[:KMID, :].T.astype(BF16)
        to_rows = jnp.where(place_mid(C2, 0) == iota((C2, C2), 1), 1.0, 0.0).astype(BF16)
        for t in range(9):
            w3_mid[s, C2 * t : C2 * (t + 1), :] = dot(to_rows, third2[s, t]).astype(BF16)

    def prepare_top(s):
        for i in range(3):
            weight_loads[3 * STEPS2 + 3 * s + i].wait()
        w2_top[s] = second3[s].T
        for t in range(9):
            tall[24 * t : 24 * (t + 1), :] = first3[s, t].astype(F32)
            w3_top[s, C3 * t : C3 * (t + 1), :] = third3[s, t]
        tall[216:217, :] = small3[5][s : s + 1].astype(F32)
        tall[217:, :] = jnp.zeros((KTOP - 217, HID), F32)
        w1_top[s] = tall[...].T.astype(BF16)

    prepare_small()
    prepare_mid(0)

    for edge in range(REACH + 1):
        blocks = REACH + 1 + edge

        def meet(blocks=blocks):
            pl.semaphore_wait(barrier, CHAN * blocks - 1 + ROWS - blocks)

        if edge < REACH:
            pl.when((r == edge) | (r == ROWS - 1 - edge))(meet)
        else:
            pl.when((r >= edge) & (r <= ROWS - 1 - edge))(meet)

    def row_copy(d, k):
        to = (c + k) % CHAN
        return pltpu.make_async_remote_copy(
            src_ref=packed.at[to],
            dst_ref=arrived.at[8 * (REACH - d) + c],
            send_sem=send_sem,
            recv_sem=recv_sem.at[REACH - d],
            device_id={"rows": r + d, "chan": to},
            device_id_type=MESH,
        )

    def sends(d, body):
        if d == REACH:
            pl.when((r + d < ROWS) & (c >= 2))(body)
        elif d == -REACH:
            pl.when((r + d >= 0) & (c < CHAN - 2))(body)
        else:
            in_image(d, body)

    for d in sorted(near, key=lambda d: -abs(d)):

        def send(d=d):
            for k in range(1 if d == 0 else 0, CHAN):
                row_copy(d, k).start()

        sends(d, send)
    arrived[8 * REACH + c] = packed[c]

    for s in range(1, STEPS2):
        prepare_mid(s)
    for s in range(STEPS3):
        prepare_top(s)

    for d in near:

        def receive(d=d):
            first, last = 8 * (d + REACH), 8 * (d + REACH) + 8
            if d == -REACH:
                first += 2
            elif abs(d) == REACH:
                last -= 2
            elif d == 0:
                last -= 1
            tiles = arrived.at[pl.ds(first, last - first)]
            pltpu.make_async_copy(tiles, tiles, recv_sem.at[d + REACH]).wait()

        in_image(d, receive)

    rows_of_lanes = []
    for k in range(3):
        lanes_of_k = []
        for g in range(WIDE // LANES):
            tile = None
            for j in range(4):
                part = roll(arrived[4 * g + j], COLS * (j - k))
                tile = part if tile is None else jnp.where(group == j, part, tile)
            lanes_of_k.append(tile)
        rows_of_lanes.append(jnp.concatenate(lanes_of_k, axis=1))
    state = jnp.concatenate(rows_of_lanes + [ones_block(WIDE, 8, 0)], axis=0)

    own = slice(NARROW // 2 - LANES, NARROW // 2 + LANES)
    loglik_terms = jnp.zeros((16, 2 * LANES), F32)
    for s in range(STEPS2):
        n = WIDE if s == 0 else NARROW
        row = iota((1, n), 1) // COLS + (0 if s == 0 else 4) + 8 * (r - REACH)
        inside = (row >= 0) & (row < 8 * ROWS)
        u = split_mix(mix2[s], state)
        q = jnp.where(inside, u[:16], 0.0)
        out = conditioner(
            q, inside, COLS, w1_mid.at[s], w2_mid.at[s], b2_mid.at[s], w3_mid.at[s], bias2[s]
        )
        if s == 0:
            u, out = u[:, LANES:-LANES], out[:, LANES:-LANES]
        sigmoid, log_sigmoid = gate(out[:16])
        loglik_terms += jnp.where(iota((16, 2 * LANES), 0) < 12, log_sigmoid[:, own], 0.0)
        lower_half = iota((8, 1), 0) < 4
        mixed = (u[8:16] + out[8:16]) * pltpu.roll(sigmoid[8:16], 4, 0)
        mixed = jnp.where(lower_half, u[8:16], mixed)
        rest = (u[16:24] + out[16:24]) * sigmoid[:8]
        state = jnp.concatenate([u[:8], mixed, rest, ones_block(NARROW, 8, 0)], axis=0)

    latent = state[:16, own]
    loglik_terms -= jnp.where(iota((16, 2 * LANES), 0) < 12, 0.5 * latent * latent, 0.0)
    for half in range(2):
        sent_latent[half] = latent[:, LANES * half : LANES * (half + 1)]

    kept = jnp.concatenate([state[16:24], state[8:16]], axis=0)
    lane, to = iota((2 * LANES, 2 * LANES), 0), iota((2 * LANES, 2 * LANES), 1)
    p, col = lane // COLS, lane % COLS
    place = (2 * (p % 2) + col % 2) * 64 + (p // 2) * 16 + col // 2
    permutation = jnp.where(place == to, 1.0, 0.0).astype(BF16)
    streams = []
    for block in range(3):
        rest = kept[:, LANES * (1 + 2 * block) : LANES * (3 + 2 * block)]
        for _ in range(3):
            high = rest.astype(BF16)
            streams.append(high)
            rest = rest - high.astype(F32)
    moved = dot(jnp.concatenate(streams, axis=0), permutation)
    blocks = [
        moved[48 * b : 48 * b + 16] + moved[48 * b + 16 : 48 * b + 32] + moved[48 * b + 32 : 48 * b + 48]
        for b in range(3)
    ]
    lane64 = iota((16, LANES), 1) < 64
    squeezed = []
    for ij in range(4):
        half = LANES * (ij // 2)
        at = [b[:, half : half + LANES] for b in blocks]
        if ij % 2 == 0:
            left, right = jnp.where(lane64, at[0], roll(at[1], 64)), at[2]
        else:
            left, right = jnp.where(lane64, roll(at[0], 64), at[1]), roll(at[2], 64)
        squeezed.append(jnp.concatenate([left, right], axis=1))
    state = jnp.concatenate(squeezed + [ones_block(NTOP, 16, 0)], axis=0)

    def latent_copy(k):
        to = (c + k) % CHAN
        return pltpu.make_async_remote_copy(
            src_ref=sent_latent.at[to // 4],
            dst_ref=got_latent.at[c],
            send_sem=latent_send,
            recv_sem=latent_recv,
            device_id={"chan": to},
            device_id_type=MESH,
        )

    for k in range(1, CHAN):
        latent_copy(k).start()
    got_latent[c] = sent_latent[c // 4]

    row = iota((1, NTOP), 1) // 16
    inside = (row + 4 * r >= 4) & (row + 4 * r < 4 * ROWS + 4) & (row < 12)
    own_top = (iota((1, LANES), 1) >= 64)
    top_terms = jnp.zeros((24, LANES), F32)
    for s in range(STEPS3):
        u = split_mix(mix3[s], state)
        q = jnp.where(inside, u[:24], 0.0)
        out = conditioner(
            q, inside, 16, w1_top.at[s], w2_top.at[s], b2_top.at[s], w3_top.at[s], bias3[s]
        )
        sigmoid, log_sigmoid = gate(out[:24])
        top_terms += log_sigmoid[:, :LANES]
        rest = (u[24:] + out[24:]) * sigmoid
        state = jnp.concatenate([u[:24], rest, ones_block(NTOP, 32, 0)], axis=0)
    z = state[:C3, :LANES]
    squares = z * z
    top_terms = jnp.where(own_top, top_terms - 0.5 * (squares[:24] + squares[24:]), 0.0)

    logdets = 256.0 * (jnp.sum(small2[1][...]) + jnp.sum(small2[4][...]))
    logdets += 64.0 * (jnp.sum(small3[1][...]) + jnp.sum(small3[4][...]))
    total = jnp.sum(loglik_terms) + jnp.sum(top_terms) + logdets
    total = (total - 0.5 * LOG_TWO_PI * (12 * 256 + 48 * 64)) * (1.0 / DIMS)
    terms[r] = jnp.full((1, LANES), total, F32)

    def term_copy(k):
        return pltpu.make_async_remote_copy(
            src_ref=terms.at[r],
            dst_ref=terms.at[r],
            send_sem=term_send,
            recv_sem=term_recv,
            device_id={"rows": (r + k) % ROWS},
            device_id_type=MESH,
        )

    for k in range(1, ROWS):
        term_copy(k).start()

    latent_top[0] = z.T[64:].reshape(4, 16, C3)

    others = got_latent.at[pl.ds(0, CHAN - 1)]
    pltpu.make_async_copy(others, others, latent_recv).wait()
    for i in range(8):
        turned = pltpu.roll(got_latent[i], (LANES - COLS * (c % 4)) % LANES, 1)
        latent_mid[i] = turned[:12, :COLS]

    others = terms.at[pl.ds(0, ROWS - 1)]
    pltpu.make_async_copy(others, others, term_recv).wait()
    whole = terms[0]
    for i in range(1, ROWS):
        whole = whole + terms[i]
    loglik[...] = whole

    pltpu.make_async_copy(others, others, term_send).wait()
    others = got_latent.at[pl.ds(0, CHAN - 1)]
    pltpu.make_async_copy(others, others, latent_send).wait()
    for d in near:

        def left_here(d=d):
            tiles = packed.at[pl.ds(0, CHAN - 1 if d == 0 else CHAN)]
            pltpu.make_async_copy(tiles, tiles, send_sem).wait()

        sends(d, left_here)


def body(*given):
    given = list(given)
    given[0] = given[0].reshape(8, C2, COLS)
    given[10] = given[10].transpose(0, 1, 3, 2)
    given[21] = given[21].transpose(0, 1, 3, 2)

    def small(n, steps):
        return (
            pltpu.VMEM((steps, n), F32),
            pltpu.VMEM((steps, n), F32),
            pltpu.VMEM((steps, n, n), F32),
            pltpu.VMEM((steps, n, n), F32),
            pltpu.VMEM((steps, n), F32),
            pltpu.VMEM((steps, HID), BF16),
            pltpu.VMEM((steps, HID), F32),
            pltpu.VMEM((steps, n), F32),
        )

    latent_mid, latent_top, loglik = pl.pallas_call(
        kernel,
        out_shape=(
            jax.ShapeDtypeStruct((8, 12, COLS), F32),
            jax.ShapeDtypeStruct((1, 4, 16, C3), F32),
            jax.ShapeDtypeStruct((1, LANES), F32),
        ),
        in_specs=[pl.BlockSpec(memory_space=pl.ANY)] * 23,
        out_specs=tuple(pl.BlockSpec(memory_space=pltpu.VMEM) for _ in range(3)),
        scratch_shapes=[
            pltpu.VMEM((8, C2, COLS), F32),
            pltpu.VMEM((8, 8, LANES), F32),
            pltpu.VMEM((8 * BLOCKS, 8, LANES), F32),
            pltpu.VMEM((STEPS2, 9, 12, HID), BF16),
            pltpu.VMEM((STEPS2, HID, HID), BF16),
            pltpu.VMEM((STEPS2, 9, C2, HID), BF16),
            pltpu.VMEM((STEPS3, 9, 24, HID), BF16),
            pltpu.VMEM((STEPS3, HID, HID), BF16),
            pltpu.VMEM((STEPS3, 9, C3, HID), BF16),
            small(C2, STEPS2),
            small(C3, STEPS3),
            pltpu.VMEM((STEPS2, C2, 96), BF16),
            pltpu.VMEM((STEPS3, C3, 240), BF16),
            pltpu.VMEM((STEPS2, C2, 1), F32),
            pltpu.VMEM((STEPS3, C3, 1), F32),
            pltpu.VMEM((KTOP, HID), F32),
            pltpu.VMEM((STEPS2, HID, KMID), BF16),
            pltpu.VMEM((STEPS2, HID, HID), BF16),
            pltpu.VMEM((STEPS2, HID, LANES), F32),
            pltpu.VMEM((STEPS2, 9 * C2, HID), BF16),
            pltpu.VMEM((STEPS3, HID, KTOP), BF16),
            pltpu.VMEM((STEPS3, HID, HID), BF16),
            pltpu.VMEM((STEPS3, HID, LANES), F32),
            pltpu.VMEM((STEPS3, 9 * C3, HID), BF16),
            pltpu.VMEM((2, 16, LANES), F32),
            pltpu.VMEM((CHAN, 16, LANES), F32),
            pltpu.VMEM((ROWS, 1, LANES), F32),
            pltpu.SemaphoreType.DMA,
            pltpu.SemaphoreType.DMA((16,)),
            pltpu.SemaphoreType.DMA((15,)),
            pltpu.SemaphoreType.DMA,
            pltpu.SemaphoreType.DMA((BLOCKS,)),
            pltpu.SemaphoreType.DMA,
            pltpu.SemaphoreType.DMA,
            pltpu.SemaphoreType.DMA,
            pltpu.SemaphoreType.DMA,
        ],
        compiler_params=pltpu.CompilerParams(collective_id=0, has_side_effects=True, vmem_limit_bytes=60 * 2**20),
    )(*given)
    return (
        latent_mid.reshape(8, 12, 1, COLS),
        latent_top.transpose(0, 3, 1, 2),
        loglik[0, :1],
    )


def solution(mesh):
    placed = (P("batch", None, ("rows", "chan"), None),) + (P(),) * 22
    return jax.shard_map(
        body,
        mesh=mesh,
        in_specs=placed,
        out_specs=(
            P("batch", None, ("rows", "chan"), None),
            P(("batch", "chan"), None, "rows", None),
            P(("batch", "chan")),
        ),
        check_vma=False,
    )
```

```python
import math

import jax
import jax.numpy as jnp
from jax import lax
from jax.experimental import pallas as pl
from jax.experimental.pallas import tpu as pltpu
from jax.sharding import PartitionSpec as P

MESH = pl.DeviceIdType.MESH
F32 = jnp.float32
BF16 = jnp.bfloat16
LOG_TWO_PI = math.log(2.0 * math.pi)

HID = 512
ROWS = 8
CHAN = 8
C2, C3 = 24, 48
STEPS2, STEPS3 = 3, 2
COLS = 32
LANES = 128
REACH = 2
BLOCKS = 2 * REACH + 1
WIDE = BLOCKS * 8 * COLS
NARROW = WIDE - 2 * LANES
KMID = 160
KTOP = 224
NTOP = 256
DIMS = 24 * 64 * 32


def iota(shape, dim):
    return lax.broadcasted_iota(jnp.int32, shape, dim)


def dot(a, b):
    return jnp.dot(a, b, preferred_element_type=F32)


def exact_dot(a, b):
    return jnp.dot(a, b, preferred_element_type=F32, precision=lax.Precision.HIGHEST)


def column(row):
    n = row.shape[1]
    eye = iota((n, n), 0) == iota((n, n), 1)
    return jnp.sum(jnp.where(eye, row, 0.0), axis=1, keepdims=True)


def place_mid(n, dim):
    at = iota((n, n), dim)
    return jnp.where(at < 12, at, jnp.where(at < 16, at + 8, at - 4))


def mixing(shift, gain, lower, upper, diag):
    n = shift.shape[1]
    i, j = iota((n, n), 0), iota((n, n), 1)
    low = jnp.where(j < i, lower, 0.0) + jnp.where(i == j, 1.0, 0.0)
    up = jnp.where(j > i, upper, 0.0) + jnp.where(i == j, jnp.exp(diag), 0.0)
    a = exact_dot(low, up) * jnp.exp(gain)
    return a, jnp.sum(a * shift, axis=1, keepdims=True)


def stacked(a, b, width, bias_at):
    rows, n = a.shape
    if width > n:
        a = jnp.concatenate([a, jnp.zeros((rows, width - n), F32)], axis=1)
    a = jnp.where(iota((rows, width), 1) == bias_at, b, a)
    high = a.astype(BF16).astype(F32)
    low = a - high
    return jnp.concatenate([high, high, low], axis=1).astype(BF16)


def split_mix(a, v):
    high = v.astype(BF16)
    low = (v - high.astype(F32)).astype(BF16)
    return dot(a, jnp.concatenate([high, low, high], axis=0))


def roll(x, by):
    n = x.shape[1]
    by = by % n
    return x if by == 0 else pltpu.roll(x, by, 1)


def ones_block(n, height, at):
    return jnp.where(iota((height, n), 0) == at, 1.0, 0.0)


def turned(x, by):
    return pltpu.roll(x, -by % LANES, 1)


def moved(blocks, j, by, lane):
    if by == 0:
        return blocks(j, 0)
    here, beside = blocks(j, by), blocks(j + (1 if by > 0 else -1), by)
    if beside is None:
        return here
    return jnp.where(lane < LANES - by, here, beside) if by > 0 else jnp.where(lane >= -by, here, beside)


def cached(get):
    kept = {}

    def blocks(j, by):
        if (j, by) not in kept:
            x = get(j)
            kept[j, by] = x if x is None or by == 0 else turned(x, by)
        return kept[j, by]

    return blocks


class Step:
    def __init__(self, first, last, width, half, inside, mix, w1, w2, b2, w3, b3, scratch):
        self.first, self.last, self.width, self.half = first, last, width, half
        self.inside, self.mix_w, self.w1, self.w2, self.b2, self.w3, self.b3 = inside, mix, w1, w2, b2, w3, b3
        self.patches, self.h1, self.h2, self.z = scratch
        self.outs = w3.shape[0] // 9
        self.u, self.q = {}, {}
        self.lane = iota((1, LANES), 1)
        col = self.lane % width
        self.edge = {-1: col > 0, 1: col < width - 1}
        self.q_blocks = cached(lambda j: self.q.get(j))
        self.z_blocks = [
            cached(lambda j, t=t: self.z_block(t, j)) for t in range(9)
        ]

    def tiles(self):
        return (self.last - self.first) // 2

    def pair(self, t):
        return self.first + 2 * t, self.first + 2 * t + 1

    def lanes(self, t):
        return slice(2 * LANES * t, 2 * LANES * (t + 1))

    def mix(self, t, state):
        pair = self.pair(t)
        u = split_mix(self.mix_w[...], jnp.concatenate([state(j) for j in pair], axis=1))
        rows = 16 if self.half == 12 else 24
        for i, j in enumerate(pair):
            self.u[j] = u[:, LANES * i : LANES * (i + 1)]
            self.q[j] = jnp.where(self.inside(j), self.u[j][:rows], 0.0)
            if rows == 16:
                self.q[j] = self.q[j].astype(BF16)

    def patch(self, t):
        taps = []
        for dy in (-1, 0, 1):
            for dx in (-1, 0, 1):
                parts = []
                for j in self.pair(t):
                    part = moved(self.q_blocks, j, self.width * dy + dx, self.lane)
                    parts.append(jnp.where(self.edge[dx], part, jnp.zeros_like(part)) if dx else part)
                taps.append(jnp.concatenate(parts, axis=1))
        if self.half == 12:
            for i, tap in enumerate(taps):
                self.patches[16 * i : 16 * (i + 1), self.lanes(t)] = tap
        else:
            taps.append(ones_block(2 * LANES, 8, 0))
            self.patches[:, self.lanes(t)] = jnp.concatenate(taps, axis=0).astype(BF16)

    def one(self, t):
        self.h1[:, self.lanes(t)] = jnp.maximum(dot(self.w1[...], self.patches[:, self.lanes(t)]), 0.0).astype(BF16)

    def two(self, t):
        bias = jnp.concatenate([self.b2[...]] * 2, axis=1)
        self.h2[:, self.lanes(t)] = jnp.maximum(dot(self.w2[...], self.h1[:, self.lanes(t)]) + bias, 0.0).astype(BF16)

    def three(self, t):
        inside = jnp.concatenate([self.inside(j) for j in self.pair(t)], axis=1)
        self.z[:, self.lanes(t)] = jnp.where(inside, dot(self.w3[...], self.h2[:, self.lanes(t)]), 0.0)

    def z_block(self, tap, j):
        if not self.first <= j < self.last:
            return None
        at = LANES * (j - self.first)
        return self.z[self.outs * tap : self.outs * (tap + 1), at : at + LANES]

    def out(self, j):
        total = self.b3[...]
        for dx in (0, -1, 1):
            side = None
            for dy in (-1, 0, 1):
                part = moved(self.z_blocks[3 * (dy + 1) + dx + 1], j, self.width * dy + dx, self.lane)
                side = part if side is None else side + part
            total = total + (jnp.where(self.edge[dx], side, 0.0) if dx else side)
        return total


def gate(g):
    small = jnp.exp(-jnp.abs(g))
    sigmoid = jnp.where(g >= 0.0, 1.0, small) / (1.0 + small)
    return sigmoid, jnp.minimum(g, 0.0) - jnp.log(1.0 + small)


STARTS = (0, 20, 40)


def wavefront(tiles, lag, starts):
    slots = []
    for s, (n, start) in enumerate(zip(tiles, starts)):
        for t in range(n):
            for part, after in enumerate(lag):
                slots.append((start + t + after, part, s, t))
    return [(s, part, t) for _, part, s, t in sorted(slots, key=lambda x: (x[0], LATE[x[1]], x[2]))]


LATE = (0, 1, 2, 3, 4, 5)
ORDER = wavefront((5, 4, 4), (0, 1, 2, 3, 4, 5), STARTS)


def kernel(
    images,
    shift_mid,
    gain_mid,
    lower_mid,
    upper_mid,
    diag_mid,
    first_mid,
    first_bias_mid,
    second_mid,
    second_bias_mid,
    third_mid,
    third_bias_mid,
    shift_top,
    gain_top,
    lower_top,
    upper_top,
    diag_top,
    first_top,
    first_bias_top,
    second_top,
    second_bias_top,
    third_top,
    third_bias_top,
    latent_mid,
    latent_top,
    loglik,
    pictures,
    packed,
    packed_half,
    arrived,
    own_rows,
    first2,
    second2,
    third2,
    first3,
    second3,
    third3,
    small2,
    small3,
    mix2,
    mix3,
    bias2,
    bias3,
    tall,
    w1_mid,
    w2_mid,
    b2_mid,
    w3_mid,
    w1_top,
    w2_top,
    b2_top,
    w3_top,
    sent_latent,
    got_latent,
    terms,
    scratch_mid,
    scratch_top,
    load_sem,
    small_sem,
    weight_sem,
    send_sem,
    recv_sem,
    latent_send,
    latent_recv,
    term_send,
    term_recv,
):
    r, c = lax.axis_index("rows"), lax.axis_index("chan")
    barrier = pltpu.get_barrier_semaphore()

    picture_load = pltpu.make_async_copy(images, pictures, load_sem)
    picture_load.start()
    given2 = (shift_mid, gain_mid, lower_mid, upper_mid, diag_mid, first_bias_mid, second_bias_mid, third_bias_mid)
    given3 = (shift_top, gain_top, lower_top, upper_top, diag_top, first_bias_top, second_bias_top, third_bias_top)
    small_loads = [
        pltpu.make_async_copy(src, dst, small_sem.at[i])
        for i, (src, dst) in enumerate(zip(given2 + given3, small2 + small3))
    ]
    weight_loads = []
    for s in range(STEPS2):
        for src, dst in ((second_mid, second2), (first_mid, first2), (third_mid, third2)):
            weight_loads.append(
                pltpu.make_async_copy(src.at[s], dst.at[s], weight_sem.at[len(weight_loads)])
            )
    for s in range(STEPS3):
        for src, dst in ((second_top, second3), (first_top, first3), (third_top, third3)):
            weight_loads.append(
                pltpu.make_async_copy(src.at[s], dst.at[s], weight_sem.at[len(weight_loads)])
            )
    def in_image(d, body):
        if d == 0:
            body()
        else:
            pl.when((r + d >= 0) & (r + d < ROWS))(body)

    near = range(-REACH, REACH + 1)

    arrived[...] = jnp.zeros_like(arrived)
    for d in near:

        def greet(d=d):
            for k in range(1 if d == 0 else 0, CHAN):
                pl.semaphore_signal(
                    barrier, 1, device_id={"rows": r + d, "chan": (c + k) % CHAN}, device_id_type=MESH
                )

        in_image(d, greet)
    for d in range(REACH + 1, ROWS):
        for far in (-d, d):

            def greet_far(far=far):
                pl.semaphore_signal(barrier, 1, device_id={"rows": r + far}, device_id_type=MESH)

            in_image(far, greet_far)

    picture_load.wait()
    for load in small_loads + weight_loads:
        load.start()
    group = iota((8, LANES), 1) // COLS
    for i in range(8):
        tile = jnp.zeros((8, LANES), F32)
        for k in range(3):
            part = pictures[i, 8 * k : 8 * k + 8, :]
            part = jnp.concatenate([part, jnp.zeros((8, LANES - COLS), F32)], axis=1)
            tile = jnp.where(group == k, roll(part, COLS * k), tile)
        packed[i] = tile
        packed_half[i] = tile.astype(BF16)

    def prepare_small():
        for load in small_loads:
            load.wait()
        shift, gain, lower, upper, diag, _, second_b, third_b = small2
        for s in range(STEPS2):
            a, b = mixing(shift[s : s + 1], gain[s : s + 1], lower[s], upper[s], diag[s : s + 1])
            to_rows = jnp.where(place_mid(C2, 0) == iota((C2, C2), 1), 1.0, 0.0)
            a = exact_dot(to_rows, a)
            if s:
                to_columns = jnp.where(place_mid(C2, 1) == iota((C2, C2), 0), 1.0, 0.0)
                a = exact_dot(a, to_columns)
            b = exact_dot(to_rows, b)
            mix2[s] = stacked(a, b, 32, C2)
            extra = third_b[s : s + 1] + jnp.where(iota((1, C2), 1) < C2 // 2, 2.0, 0.0)
            bias2[s] = jnp.sum(to_rows * extra, axis=1, keepdims=True)
            b2_mid[s] = jnp.broadcast_to(second_b[s : s + 1], (LANES, HID)).T
        shift, gain, lower, upper, diag, _, second_b, third_b = small3
        for s in range(STEPS3):
            a, b = mixing(shift[s : s + 1], gain[s : s + 1], lower[s], upper[s], diag[s : s + 1])
            if s == 0:
                n, k = iota((C3, 64), 0), iota((C3, 64), 1)
                row = n // 4
                at = (n % 4) * 16 + jnp.where(row < 8, row, row + 4)
                a = exact_dot(a, jnp.where(at == k, 1.0, 0.0))
                mix3[s] = stacked(a, b, 80, 64)
            else:
                mix3[s] = stacked(a, b, 80, C3)
            extra = third_b[s : s + 1] + jnp.where(iota((1, C3), 1) < C3 // 2, 2.0, 0.0)
            bias3[s] = column(extra)
            b2_top[s] = jnp.broadcast_to(second_b[s : s + 1], (LANES, HID)).T

    def prepare_mid(s):
        for i in range(3):
            weight_loads[3 * s + i].wait()
        w2_mid[s] = second2[s].T
        tall[...] = jnp.zeros_like(tall)
        for t in range(9):
            tall[16 * t : 16 * t + 12, :] = first2[s, t].astype(F32)
        tall[144:145, :] = small2[5][s : s + 1].astype(F32)
        w1_mid[s] = tall[:KMID, :].T.astype(BF16)
        to_rows = jnp.where(place_mid(C2, 0) == iota((C2, C2), 1), 1.0, 0.0).astype(BF16)
        for t in range(9):
            w3_mid[s, C2 * t : C2 * (t + 1), :] = dot(to_rows, third2[s, t]).astype(BF16)

    def prepare_top(s):
        for i in range(3):
            weight_loads[3 * STEPS2 + 3 * s + i].wait()
        w2_top[s] = second3[s].T
        for t in range(9):
            tall[24 * t : 24 * (t + 1), :] = first3[s, t].astype(F32)
            w3_top[s, C3 * t : C3 * (t + 1), :] = third3[s, t]
        tall[216:217, :] = small3[5][s : s + 1].astype(F32)
        tall[217:, :] = jnp.zeros((KTOP - 217, HID), F32)
        w1_top[s] = tall[...].T.astype(BF16)

    for edge in range(REACH + 1):
        blocks = REACH + 1 + edge

        def meet(blocks=blocks):
            pl.semaphore_wait(barrier, CHAN * blocks - 1 + ROWS - blocks)

        if edge < REACH:
            pl.when((r == edge) | (r == ROWS - 1 - edge))(meet)
        else:
            pl.when((r >= edge) & (r <= ROWS - 1 - edge))(meet)

    def row_copy(d, k):
        to = (c + k) % CHAN
        return pltpu.make_async_remote_copy(
            src_ref=packed_half.at[to] if d else packed.at[to],
            dst_ref=arrived.at[8 * (REACH - d) + c] if d else own_rows.at[c],
            send_sem=send_sem,
            recv_sem=recv_sem.at[REACH - d],
            device_id={"rows": r + d, "chan": to},
            device_id_type=MESH,
        )

    def sends(d, body):
        if d == REACH:
            pl.when((r + d < ROWS) & (c >= 2))(body)
        elif d == -REACH:
            pl.when((r + d >= 0) & (c < CHAN - 2))(body)
        else:
            in_image(d, body)

    for d in sorted(near, key=lambda d: -abs(d)):

        def send(d=d):
            for k in range(1 if d == 0 else 0, CHAN):
                row_copy(d, k).start()

        sends(d, send)
    own_rows[c] = packed[c]

    prepare_small()
    for s in range(STEPS2):
        prepare_mid(s)
    for s in range(STEPS3):
        prepare_top(s)

    for d in near:

        def receive(d=d):
            first, last = 8 * (d + REACH), 8 * (d + REACH) + 8
            if d == -REACH:
                first += 2
            elif abs(d) == REACH:
                last -= 2
            tiles = arrived.at[pl.ds(first, last - first)] if d else own_rows.at[pl.ds(0, CHAN - 1)]
            pltpu.make_async_copy(tiles, tiles, recv_sem.at[d + REACH]).wait()

        in_image(d, receive)

    lane128 = iota((1, LANES), 1)
    for which in range(2):
        spare = iota((16, WIDE), 0) == 0
        scratch_mid[which][0][9 * 16 :, :] = jnp.where(spare, 1.0, 0.0).astype(BF16)

    def inside_mid(j):
        row = lane128 // COLS + 4 * j + 8 * (r - REACH)
        return (row >= 0) & (row < 8 * ROWS)

    def unpacked(g):
        rows = []
        for k in range(3):
            tile = None
            for j in range(4):
                at = 4 * g + j
                part = own_rows[at - 16] if 16 <= at < 24 else arrived[at].astype(F32)
                part = turned(part, COLS * (k - j))
                tile = part if tile is None else jnp.where(group == j, part, tile)
            rows.append(tile)
        return jnp.concatenate(rows + [ones_block(LANES, 8, 0)], axis=0)

    steps = []
    for s in range(STEPS2):
        first, last = (0, WIDE // LANES) if s == 0 else (1, WIDE // LANES - 1)
        steps.append(
            Step(
                first, last, COLS, 12, inside_mid, mix2.at[s],
                w1_mid.at[s], w2_mid.at[s], b2_mid.at[s], w3_mid.at[s], bias2.at[s], scratch_mid[s % 2],
            )
        )
    states = [{} for _ in range(STEPS2 + 1)]
    own = (4, 5)
    loglik_terms = []

    def finish(s, j):
        step = steps[s]
        u, out = step.u[j], step.out(j)
        sigmoid, log_sigmoid = gate(out[:16])
        if j in own:
            loglik_terms.append(log_sigmoid)
        mixed = (u[8:16] + out[8:16]) * pltpu.roll(sigmoid[8:16], 4, 0)
        mixed = jnp.where(iota((8, 1), 0) < 4, u[8:16], mixed)
        rest = (u[16:24] + out[16:24]) * sigmoid[:8]
        states[s + 1][j] = jnp.concatenate([u[:8], mixed, rest, ones_block(LANES, 8, 0)], axis=0)

    for s, part, t in ORDER:
        step = steps[s]
        if part == 0:
            for j in step.pair(t):
                if s == 0:
                    states[0][j] = unpacked(j)
            step.mix(t, lambda j: states[s][j])
        elif part == 1:
            step.patch(t)
        elif part == 2:
            step.one(t)
        elif part == 3:
            step.two(t)
        elif part == 4:
            step.three(t)
        else:
            for j in step.pair(t):
                if s == STEPS2 - 1 or 1 <= j < WIDE // LANES - 1:
                    finish(s, j)

    final = states[STEPS2]
    for half in range(2):
        latent = final[own[half]][:16]
        loglik_terms.append(-0.5 * latent * latent)
        sent_latent[half] = latent
    loglik_sum = jnp.where(iota((16, LANES), 0) < 12, sum(loglik_terms), 0.0)

    lane, to = iota((2 * LANES, 2 * LANES), 0), iota((2 * LANES, 2 * LANES), 1)
    p, col = lane // COLS, lane % COLS
    place = (2 * (p % 2) + col % 2) * 64 + (p // 2) * 16 + col // 2
    permutation = jnp.where(place == to, 1.0, 0.0).astype(BF16)
    streams = []
    for block in range(3):
        pair = [final[2 + 2 * block], final[3 + 2 * block]]
        rest = jnp.concatenate([jnp.concatenate([x[16:24], x[8:16]], axis=0) for x in pair], axis=1)
        for _ in range(3):
            high = rest.astype(BF16)
            streams.append(high)
            rest = rest - high.astype(F32)
    apart = dot(jnp.concatenate(streams, axis=0), permutation)
    blocks = [
        apart[48 * b : 48 * b + 16] + apart[48 * b + 16 : 48 * b + 32] + apart[48 * b + 32 : 48 * b + 48]
        for b in range(3)
    ]
    lane64 = iota((16, LANES), 1) < 64
    squeezed = []
    for ij in range(4):
        half = LANES * (ij // 2)
        at = [b[:, half : half + LANES] for b in blocks]
        if ij % 2 == 0:
            left, right = jnp.where(lane64, at[0], roll(at[1], 64)), at[2]
        else:
            left, right = jnp.where(lane64, roll(at[0], 64), at[1]), roll(at[2], 64)
        squeezed.append(jnp.concatenate([left, right], axis=1))
    state = jnp.concatenate(squeezed + [ones_block(NTOP, 16, 0)], axis=0)

    def latent_copy(k):
        to = (c + k) % CHAN
        return pltpu.make_async_remote_copy(
            src_ref=sent_latent.at[to // 4],
            dst_ref=got_latent.at[c],
            send_sem=latent_send,
            recv_sem=latent_recv,
            device_id={"chan": to},
            device_id_type=MESH,
        )

    for k in range(1, CHAN):
        latent_copy(k).start()
    got_latent[c] = sent_latent[c // 4]

    def inside_top(j):
        row = lane128 // 16 + 8 * j
        return (row + 4 * r >= 4) & (row + 4 * r < 4 * ROWS + 4) & (row < 12)

    own_top = lane128 >= 64
    top_terms = jnp.zeros((24, LANES), F32)
    for s in range(STEPS3):
        step = Step(
            0, 2, 16, 24, inside_top, mix3.at[s],
            w1_top.at[s], w2_top.at[s], b2_top.at[s], w3_top.at[s], bias3.at[s], scratch_top,
        )
        step.mix(0, lambda j: state[:, LANES * j : LANES * (j + 1)])
        step.patch(0)
        step.one(0)
        step.two(0)
        step.three(0)
        blocks = []
        for j in range(2 if s == 0 else 1):
            u, out = step.u[j], step.out(j)
            sigmoid, log_sigmoid = gate(out[:24])
            if j == 0:
                top_terms += log_sigmoid
            blocks.append(jnp.concatenate([u[:24], (u[24:] + out[24:]) * sigmoid, ones_block(LANES, 32, 0)], axis=0))
        state = jnp.concatenate(blocks, axis=1)
    z = state[:C3, :LANES]
    squares = z * z
    top_terms = jnp.where(own_top, top_terms - 0.5 * (squares[:24] + squares[24:]), 0.0)

    logdets = 256.0 * (jnp.sum(small2[1][...]) + jnp.sum(small2[4][...]))
    logdets += 64.0 * (jnp.sum(small3[1][...]) + jnp.sum(small3[4][...]))
    total = jnp.sum(loglik_sum) + jnp.sum(top_terms) + logdets
    total = (total - 0.5 * LOG_TWO_PI * (12 * 256 + 48 * 64)) * (1.0 / DIMS)
    terms[r] = jnp.full((1, LANES), total, F32)

    def term_copy(k):
        return pltpu.make_async_remote_copy(
            src_ref=terms.at[r],
            dst_ref=terms.at[r],
            send_sem=term_send,
            recv_sem=term_recv,
            device_id={"rows": (r + k) % ROWS},
            device_id_type=MESH,
        )

    for k in range(1, ROWS):
        term_copy(k).start()

    latent_top[0] = z.T[64:].reshape(4, 16, C3)

    others = got_latent.at[pl.ds(0, CHAN - 1)]
    pltpu.make_async_copy(others, others, latent_recv).wait()
    for i in range(8):
        lined = pltpu.roll(got_latent[i], (LANES - COLS * (c % 4)) % LANES, 1)
        latent_mid[12 * i : 12 * i + 12, :] = lined[:12, :COLS]

    others = terms.at[pl.ds(0, ROWS - 1)]
    pltpu.make_async_copy(others, others, term_recv).wait()
    whole = terms[0]
    for i in range(1, ROWS):
        whole = whole + terms[i]
    loglik[...] = whole

    pltpu.make_async_copy(others, others, term_send).wait()
    others = got_latent.at[pl.ds(0, CHAN - 1)]
    pltpu.make_async_copy(others, others, latent_send).wait()
    for d in near:

        def left_here(d=d):
            tiles = packed_half if d else packed.at[pl.ds(0, CHAN - 1)]
            pltpu.make_async_copy(tiles, tiles, send_sem).wait()

        sends(d, left_here)


def leave(latent_mid, latent_top, loglik, latent_mid_out, latent_top_out, loglik_out, sem):
    copies = [
        pltpu.make_async_copy(src, dst, sem.at[i])
        for i, (src, dst) in enumerate(
            ((latent_mid, latent_mid_out), (latent_top, latent_top_out), (loglik, loglik_out))
        )
    ]
    for copy in copies:
        copy.start()
    for copy in copies:
        copy.wait()


def body(*given):
    given = list(given)
    given[0] = given[0].reshape(8, C2, COLS)
    given[10] = given[10].transpose(0, 1, 3, 2)
    given[21] = given[21].transpose(0, 1, 3, 2)

    def small(n, steps):
        return (
            pltpu.VMEM((steps, n), F32),
            pltpu.VMEM((steps, n), F32),
            pltpu.VMEM((steps, n, n), F32),
            pltpu.VMEM((steps, n, n), F32),
            pltpu.VMEM((steps, n), F32),
            pltpu.VMEM((steps, HID), BF16),
            pltpu.VMEM((steps, HID), F32),
            pltpu.VMEM((steps, n), F32),
        )

    def inner(taps, lanes, outs):
        return (
            pltpu.VMEM((taps, lanes), BF16),
            pltpu.VMEM((HID, lanes), BF16),
            pltpu.VMEM((HID, lanes), BF16),
            pltpu.VMEM((9 * outs, lanes), F32),
        )

    latent_mid, latent_top, loglik = pl.pallas_call(
        kernel,
        out_shape=(
            pltpu.VMEM((8 * 12, COLS), F32),
            pltpu.VMEM((1, 4, 16, C3), F32),
            pltpu.VMEM((1, LANES), F32),
        ),
        in_specs=[pl.BlockSpec(memory_space=pl.ANY)] * 23,
        out_specs=tuple(pl.BlockSpec(memory_space=pltpu.VMEM) for _ in range(3)),
        scratch_shapes=[
            pltpu.VMEM((8, C2, COLS), F32),
            pltpu.VMEM((8, 8, LANES), F32),
            pltpu.VMEM((8, 8, LANES), BF16),
            pltpu.VMEM((8 * BLOCKS, 8, LANES), BF16),
            pltpu.VMEM((8, 8, LANES), F32),
            pltpu.VMEM((STEPS2, 9, 12, HID), BF16),
            pltpu.VMEM((STEPS2, HID, HID), BF16),
            pltpu.VMEM((STEPS2, 9, C2, HID), BF16),
            pltpu.VMEM((STEPS3, 9, 24, HID), BF16),
            pltpu.VMEM((STEPS3, HID, HID), BF16),
            pltpu.VMEM((STEPS3, 9, C3, HID), BF16),
            small(C2, STEPS2),
            small(C3, STEPS3),
            pltpu.VMEM((STEPS2, C2, 96), BF16),
            pltpu.VMEM((STEPS3, C3, 240), BF16),
            pltpu.VMEM((STEPS2, C2, 1), F32),
            pltpu.VMEM((STEPS3, C3, 1), F32),
            pltpu.VMEM((KTOP, HID), F32),
            pltpu.VMEM((STEPS2, HID, KMID), BF16),
            pltpu.VMEM((STEPS2, HID, HID), BF16),
            pltpu.VMEM((STEPS2, HID, LANES), F32),
            pltpu.VMEM((STEPS2, 9 * C2, HID), BF16),
            pltpu.VMEM((STEPS3, HID, KTOP), BF16),
            pltpu.VMEM((STEPS3, HID, HID), BF16),
            pltpu.VMEM((STEPS3, HID, LANES), F32),
            pltpu.VMEM((STEPS3, 9 * C3, HID), BF16),
            pltpu.VMEM((2, 16, LANES), F32),
            pltpu.VMEM((CHAN, 16, LANES), F32),
            pltpu.VMEM((ROWS, 1, LANES), F32),
            tuple(inner(KMID, WIDE, C2) for _ in range(2)),
            inner(KTOP, NTOP, C3),
            pltpu.SemaphoreType.DMA,
            pltpu.SemaphoreType.DMA((16,)),
            pltpu.SemaphoreType.DMA((15,)),
            pltpu.SemaphoreType.DMA,
            pltpu.SemaphoreType.DMA((BLOCKS,)),
            pltpu.SemaphoreType.DMA,
            pltpu.SemaphoreType.DMA,
            pltpu.SemaphoreType.DMA,
            pltpu.SemaphoreType.DMA,
        ],
        compiler_params=pltpu.CompilerParams(collective_id=0, has_side_effects=True, vmem_limit_bytes=60 * 2**20),
    )(*given)
    latent_mid, latent_top, loglik = pl.pallas_call(
        leave,
        out_shape=(
            jax.ShapeDtypeStruct((8 * 12, COLS), F32),
            jax.ShapeDtypeStruct((1, 4, 16, C3), F32),
            jax.ShapeDtypeStruct((1, LANES), F32),
        ),
        in_specs=[pl.BlockSpec(memory_space=pltpu.VMEM)] * 3,
        out_specs=tuple(pl.BlockSpec(memory_space=pl.ANY) for _ in range(3)),
        scratch_shapes=[pltpu.SemaphoreType.DMA((3,))],
    )(*(pltpu.with_memory_space_constraint(x, pltpu.VMEM) for x in (latent_mid, latent_top, loglik)))
    return (
        latent_mid.reshape(8, 12, 1, COLS),
        latent_top.transpose(0, 3, 1, 2),
        loglik[0, :1],
    )


def solution(mesh):
    placed = (P("batch", None, ("rows", "chan"), None),) + (P(),) * 22
    return jax.shard_map(
        body,
        mesh=mesh,
        in_specs=placed,
        out_specs=(
            P("batch", None, ("rows", "chan"), None),
            P(("batch", "chan"), None, "rows", None),
            P(("batch", "chan")),
        ),
        check_vma=False,
    )
```

```python
import math

import jax
import jax.numpy as jnp
from jax import lax
from jax.experimental import pallas as pl
from jax.experimental.pallas import tpu as pltpu
from jax.sharding import PartitionSpec as P

MESH = pl.DeviceIdType.MESH
F32 = jnp.float32
BF16 = jnp.bfloat16
LOG_TWO_PI = math.log(2.0 * math.pi)

HID = 512
ROWS = 8
CHAN = 8
C2, C3 = 24, 48
STEPS2, STEPS3 = 3, 2
COLS = 32
LANES = 128
REACH = 2
BLOCKS = 2 * REACH + 1
WIDE = BLOCKS * 8 * COLS
NARROW = WIDE - 2 * LANES
KMID = 160
KTOP = 224
NTOP = 256
DIMS = 24 * 64 * 32


def iota(shape, dim):
    return lax.broadcasted_iota(jnp.int32, shape, dim)


def dot(a, b):
    return jnp.dot(a, b, preferred_element_type=F32)


def exact_dot(a, b):
    return jnp.dot(a, b, preferred_element_type=F32, precision=lax.Precision.HIGHEST)


def column(row):
    n = row.shape[1]
    eye = iota((n, n), 0) == iota((n, n), 1)
    return jnp.sum(jnp.where(eye, row, 0.0), axis=1, keepdims=True)


def place_mid(n, dim):
    at = iota((n, n), dim)
    return jnp.where(at < 12, at, jnp.where(at < 16, at + 8, at - 4))


def mixing(shift, gain, lower, upper, diag):
    n = shift.shape[1]
    i, j = iota((n, n), 0), iota((n, n), 1)
    low = jnp.where(j < i, lower, 0.0) + jnp.where(i == j, 1.0, 0.0)
    up = jnp.where(j > i, upper, 0.0) + jnp.where(i == j, jnp.exp(diag), 0.0)
    a = exact_dot(low, up) * jnp.exp(gain)
    return a, jnp.sum(a * shift, axis=1, keepdims=True)


def stacked(a, b, width, bias_at):
    rows, n = a.shape
    if width > n:
        a = jnp.concatenate([a, jnp.zeros((rows, width - n), F32)], axis=1)
    a = jnp.where(iota((rows, width), 1) == bias_at, b, a)
    high = a.astype(BF16).astype(F32)
    low = a - high
    return jnp.concatenate([high, high, low], axis=1).astype(BF16)


def split_mix(a, v):
    high = v.astype(BF16)
    low = (v - high.astype(F32)).astype(BF16)
    return dot(a, jnp.concatenate([high, low, high], axis=0))


def roll(x, by):
    n = x.shape[1]
    by = by % n
    return x if by == 0 else pltpu.roll(x, by, 1)


def ones_block(n, height, at):
    return jnp.where(iota((height, n), 0) == at, 1.0, 0.0)


def turned(x, by):
    return pltpu.roll(x, -by % LANES, 1)


def moved(blocks, j, by, lane):
    if by == 0:
        return blocks(j, 0)
    here, beside = blocks(j, by), blocks(j + (1 if by > 0 else -1), by)
    if beside is None:
        return here
    return jnp.where(lane < LANES - by, here, beside) if by > 0 else jnp.where(lane >= -by, here, beside)


def cached(get):
    kept = {}

    def blocks(j, by):
        if (j, by) not in kept:
            x = get(j)
            kept[j, by] = x if x is None or by == 0 else turned(x, by)
        return kept[j, by]

    return blocks


def cut(rows, parts):
    each = -(-rows // parts // 8) * 8
    return [slice(at, min(at + each, rows)) for at in range(0, rows, each)]


class Step:
    def __init__(self, first, last, width, half, inside, mix, w1, w2, b2, w3, b3, scratch, per=2, wrap=None, parts=1):
        self.parts = parts
        self.first, self.last, self.width, self.half, self.per, self.wrap = first, last, width, half, per, wrap
        self.inside, self.mix_w, self.w1, self.w2, self.b2, self.w3, self.b3 = inside, mix, w1, w2, b2, w3, b3
        self.patches, self.h1, self.h2, self.z = scratch
        self.outs = w3.shape[0] // 9
        self.u, self.q = {}, {}
        self.lane = iota((1, LANES), 1)
        col = self.lane % width
        self.edge = {-1: col > 0, 1: col < width - 1}
        self.q_blocks = cached(lambda j: self.q.get(j % wrap if wrap else j))
        self.z_blocks = [
            cached(lambda j, t=t: self.z_block(t, j)) for t in range(9)
        ]

    def pair(self, t):
        return [self.first + self.per * t + i for i in range(self.per)]

    def lanes(self, t):
        return slice(self.per * LANES * t, self.per * LANES * (t + 1))

    def mix(self, t, state):
        pair = self.pair(t)
        u = split_mix(self.mix_w[...], jnp.concatenate([state(j) for j in pair], axis=1))
        self.take(t, [u[:, LANES * i : LANES * (i + 1)] for i in range(self.per)])

    def take(self, t, u):
        rows = 16 if self.half == 12 else 24
        for i, j in enumerate(self.pair(t)):
            self.u[j] = u[i]
            self.q[j] = jnp.where(self.inside(j), self.u[j][:rows], 0.0)
            if rows == 16:
                self.q[j] = self.q[j].astype(BF16)

    def patch(self, t):
        taps = []
        for dy in (-1, 0, 1):
            for dx in (-1, 0, 1):
                parts = []
                for j in self.pair(t):
                    part = moved(self.q_blocks, j, self.width * dy + dx, self.lane)
                    parts.append(jnp.where(self.edge[dx], part, jnp.zeros_like(part)) if dx else part)
                taps.append(jnp.concatenate(parts, axis=1))
        if self.half == 12:
            for i, tap in enumerate(taps):
                self.patches[16 * i : 16 * (i + 1), self.lanes(t)] = tap
        else:
            taps.append(ones_block(self.per * LANES, 8, 0))
            self.patches[:, self.lanes(t)] = jnp.concatenate(taps, axis=0).astype(BF16)

    def one(self, t):
        patches = self.patches[:, self.lanes(t)]
        for m in cut(HID, self.parts):
            self.h1[m, self.lanes(t)] = jnp.maximum(dot(self.w1[m, :], patches), 0.0).astype(BF16)

    def two(self, t):
        h1 = self.h1[:, self.lanes(t)]
        for m in cut(HID, self.parts):
            bias = jnp.concatenate([self.b2[m, :]] * self.per, axis=1)
            self.h2[m, self.lanes(t)] = jnp.maximum(dot(self.w2[m, :], h1) + bias, 0.0).astype(BF16)

    def three(self, t):
        inside = jnp.concatenate([self.inside(j) for j in self.pair(t)], axis=1)
        h2 = self.h2[:, self.lanes(t)]
        for m in cut(9 * self.outs, self.parts):
            self.z[m, self.lanes(t)] = jnp.where(inside, dot(self.w3[m, :], h2), 0.0)

    def z_block(self, tap, j):
        if self.wrap:
            j = j % self.wrap
        if not self.first <= j < self.last:
            return None
        at = LANES * (j - self.first)
        return self.z[self.outs * tap : self.outs * (tap + 1), at : at + LANES]

    def out(self, j):
        total = self.b3[...]
        for dx in (0, -1, 1):
            side = None
            for dy in (-1, 0, 1):
                part = moved(self.z_blocks[3 * (dy + 1) + dx + 1], j, self.width * dy + dx, self.lane)
                side = part if side is None else side + part
            total = total + (jnp.where(self.edge[dx], side, 0.0) if dx else side)
        return total


def gate(g):
    small = jnp.exp(-jnp.abs(g))
    sigmoid = jnp.where(g >= 0.0, 1.0, small) / (1.0 + small)
    return sigmoid, jnp.minimum(g, 0.0) - jnp.log(1.0 + small)


def emission(orders, firsts, gaps):
    slots, done = [], {}
    for s, (order, first) in enumerate(zip(orders, firsts)):
        start = gaps[s]
        near = lambda t: [x for x in (t - 1, t, t + 1) if x in order]
        at = {}
        for i, t in enumerate(order):
            need = [done[j] for j in (first + 2 * t, first + 2 * t + 1)] if s else []
            at[0, t] = max([start + i] + need)
        last = 0
        for t in order:
            at[1, t] = max(at[0, x] for x in near(t)) + 1
            at[2, t] = last = max(at[1, t], last + 1)
            at[3, t] = at[2, t] + LAG
            at[4, t] = at[2, t] + 2 * LAG
        for t in order:
            at[5, t] = max(at[4, x] for x in near(t)) + 1
            for j in (first + 2 * t, first + 2 * t + 1):
                done[j] = at[5, t]
        slots += [(slot, part, order.index(t), s, t) for (part, t), slot in at.items()]
    return [(s, part, t) for _, part, _, s, t in sorted(slots, key=lambda x: (x[0], x[3], x[1], x[2]))]


LAG = 1
MID_PARTS = 2
TOP_PARTS = 4
ORDER = emission(((0, 1, 2, 3, 4), (0, 1, 2, 3), (0, 1, 2, 3)), (0, 1, 1), (0, 0, 0))


def kernel(
    images,
    shift_mid,
    gain_mid,
    lower_mid,
    upper_mid,
    diag_mid,
    first_mid,
    first_bias_mid,
    second_mid,
    second_bias_mid,
    third_mid,
    third_bias_mid,
    shift_top,
    gain_top,
    lower_top,
    upper_top,
    diag_top,
    first_top,
    first_bias_top,
    second_top,
    second_bias_top,
    third_top,
    third_bias_top,
    latent_mid,
    latent_top,
    loglik,
    pictures,
    packed,
    packed_half,
    arrived,
    own_rows,
    first2,
    second2,
    third2,
    first3,
    second3,
    third3,
    small2,
    small3,
    mix2,
    mix3,
    bias2,
    bias3,
    tall,
    w1_mid,
    w2_mid,
    b2_mid,
    w3_mid,
    w1_top,
    w2_top,
    b2_top,
    w3_top,
    sent_latent,
    got_latent,
    terms,
    scratch_mid,
    scratch_top,
    load_sem,
    small_sem,
    weight_sem,
    send_sem,
    recv_sem,
    latent_send,
    latent_recv,
    term_send,
    term_recv,
):
    r, c = lax.axis_index("rows"), lax.axis_index("chan")
    barrier = pltpu.get_barrier_semaphore()

    picture_load = pltpu.make_async_copy(images, pictures, load_sem)
    picture_load.start()
    given2 = (shift_mid, gain_mid, lower_mid, upper_mid, diag_mid, first_bias_mid, second_bias_mid, third_bias_mid)
    given3 = (shift_top, gain_top, lower_top, upper_top, diag_top, first_bias_top, second_bias_top, third_bias_top)
    small_loads = [
        pltpu.make_async_copy(src, dst, small_sem.at[i])
        for i, (src, dst) in enumerate(zip(given2 + given3, small2 + small3))
    ]
    for load in small_loads:
        load.start()
    weight_loads = []
    for s in range(STEPS2):
        for src, dst in ((second_mid, second2), (first_mid, first2), (third_mid, third2)):
            weight_loads.append(
                pltpu.make_async_copy(src.at[s], dst.at[s], weight_sem.at[len(weight_loads)])
            )
    for s in range(STEPS3):
        for src, dst in ((second_top, second3), (first_top, first3), (third_top, third3)):
            weight_loads.append(
                pltpu.make_async_copy(src.at[s], dst.at[s], weight_sem.at[len(weight_loads)])
            )
    def in_image(d, body):
        if d == 0:
            body()
        else:
            pl.when((r + d >= 0) & (r + d < ROWS))(body)

    near = range(-REACH, REACH + 1)

    arrived[...] = jnp.zeros_like(arrived)
    def greet(d):
        for to in range(CHAN):

            def signal(to=to):
                pl.semaphore_signal(barrier, 1, device_id={"rows": r + d, "chan": to}, device_id_type=MESH)

            if d == 0:
                pl.when(c != to)(signal)
            else:
                signal()

    def greet_far(d):
        pl.semaphore_signal(barrier, 1, device_id={"rows": r + d}, device_id_type=MESH)

    for d in sorted(range(1 - ROWS, ROWS), key=lambda d: (abs(d) > REACH, -abs(d))):
        in_image(d, lambda d=d: greet(d) if abs(d) <= REACH else greet_far(d))

    picture_load.wait()
    def prepare_mix(s):
        shift, gain, lower, upper, diag, _, second_b, third_b = small2
        a, b = mixing(shift[s : s + 1], gain[s : s + 1], lower[s], upper[s], diag[s : s + 1])
        to_rows = jnp.where(place_mid(C2, 0) == iota((C2, C2), 1), 1.0, 0.0)
        a, b = exact_dot(to_rows, a), exact_dot(to_rows, b)
        if s:
            to_columns = jnp.where(place_mid(C2, 1) == iota((C2, C2), 0), 1.0, 0.0)
            a = exact_dot(a, to_columns)
        mix2[s] = stacked(a, b, 32, C2)
        extra = third_b[s : s + 1] + jnp.where(iota((1, C2), 1) < C2 // 2, 2.0, 0.0)
        bias2[s] = jnp.sum(to_rows * extra, axis=1, keepdims=True)

    def prepare_small():
        for s in range(STEPS2):
            if s:
                prepare_mix(s)
            b2_mid[s] = jnp.broadcast_to(small2[6][s : s + 1], (LANES, HID)).T
        shift, gain, lower, upper, diag, _, second_b, third_b = small3
        for s in range(STEPS3):
            a, b = mixing(shift[s : s + 1], gain[s : s + 1], lower[s], upper[s], diag[s : s + 1])
            if s == 0:
                n, k = iota((C3, 64), 0), iota((C3, 64), 1)
                row = n // 4
                at = (n % 4) * 16 + jnp.where(row < 8, row, row + 4)
                a = exact_dot(a, jnp.where(at == k, 1.0, 0.0))
                mix3[s] = stacked(a, b, 80, 64)
            else:
                mix3[s] = stacked(a, b, 80, C3)
            extra = third_b[s : s + 1] + jnp.where(iota((1, C3), 1) < C3 // 2, 2.0, 0.0)
            bias3[s] = column(extra)
            b2_top[s] = jnp.broadcast_to(second_b[s : s + 1], (LANES, HID)).T

    def prepare_mid(s):
        for i in range(3):
            weight_loads[3 * s + i].wait()
        w2_mid[s] = second2[s].T
        tall[...] = jnp.zeros_like(tall)
        for t in range(9):
            tall[16 * t : 16 * t + 12, :] = first2[s, t].astype(F32)
        tall[144:145, :] = small2[5][s : s + 1].astype(F32)
        w1_mid[s] = tall[:KMID, :].T.astype(BF16)
        to_rows = jnp.where(place_mid(C2, 0) == iota((C2, C2), 1), 1.0, 0.0).astype(BF16)
        for t in range(9):
            w3_mid[s, C2 * t : C2 * (t + 1), :] = dot(to_rows, third2[s, t]).astype(BF16)

    def prepare_top(s):
        for i in range(3):
            weight_loads[3 * STEPS2 + 3 * s + i].wait()
        w2_top[s] = second3[s].T
        for t in range(9):
            tall[24 * t : 24 * (t + 1), :] = first3[s, t].astype(F32)
            w3_top[s, C3 * t : C3 * (t + 1), :] = third3[s, t]
        tall[216:217, :] = small3[5][s : s + 1].astype(F32)
        tall[217:, :] = jnp.zeros((KTOP - 217, HID), F32)
        w1_top[s] = tall[...].T.astype(BF16)

    for load in small_loads:
        load.wait()
    for load in weight_loads:
        load.start()
    prepare_mix(0)
    group = iota((8, LANES), 1) // COLS
    pictures_in = []
    for half in range(2):
        rows = []
        for k in range(3):
            tile = None
            for j in range(4):
                part = pictures[4 * half + j, 8 * k : 8 * k + 8, :]
                part = jnp.concatenate([part, jnp.zeros((8, LANES - COLS), F32)], axis=1)
                part = turned(part, -COLS * j)
                tile = part if tile is None else jnp.where(group == j, part, tile)
            rows.append(tile)
        pictures_in.append(jnp.concatenate(rows + [ones_block(LANES, 8, 0)], axis=0))
    mixed_in = split_mix(mix2[0], jnp.concatenate(pictures_in, axis=1))

    for i in range(8):
        tile = jnp.zeros((8, LANES), F32)
        for k in range(3):
            part = mixed_in[8 * k : 8 * k + 8, LANES * (i // 4) : LANES * (i // 4 + 1)]
            tile = jnp.where(group == k, turned(part, COLS * (i % 4 - k)), tile)
        packed[i] = tile
        packed_half[i] = tile.astype(BF16)

    for edge in range(REACH + 1):
        blocks = REACH + 1 + edge

        def meet(blocks=blocks):
            pl.semaphore_wait(barrier, CHAN * blocks - 1 + ROWS - blocks)

        if edge < REACH:
            pl.when((r == edge) | (r == ROWS - 1 - edge))(meet)
        else:
            pl.when((r >= edge) & (r <= ROWS - 1 - edge))(meet)

    def row_copy(d, k):
        to = lax.rem(c + k, CHAN)
        return pltpu.make_async_remote_copy(
            src_ref=packed_half.at[to] if d else packed.at[to],
            dst_ref=arrived.at[8 * (REACH - d) + c] if d else own_rows.at[c],
            send_sem=send_sem,
            recv_sem=recv_sem.at[REACH - d],
            device_id={"rows": r + d, "chan": to},
            device_id_type=MESH,
        )

    def sends(d, body):
        if d == REACH:
            pl.when((r + d < ROWS) & (c >= 2))(body)
        elif d == -REACH:
            pl.when((r + d >= 0) & (c < CHAN - 2))(body)
        else:
            in_image(d, body)

    for d in sorted(near, key=lambda d: -abs(d)):

        def send(d=d):
            for k in (4, 3, 5, 2, 6, 1, 7) + (() if d == 0 else (0,)):
                row_copy(d, k).start()

        sends(d, send)
    own_rows[c] = packed[c]

    prepare_small()
    for s in range(STEPS2):
        prepare_mid(s)
    for s in range(STEPS3):
        prepare_top(s)

    def arrive(d):
        first, last = 8 * (d + REACH), 8 * (d + REACH) + 8
        if d == -REACH:
            first += 2
        elif d == REACH:
            last -= 2
        tiles = arrived.at[pl.ds(first, last - first)] if d else own_rows.at[pl.ds(0, CHAN - 1)]

        def wait():
            pltpu.make_async_copy(tiles, tiles, recv_sem.at[d + REACH]).wait()

        in_image(d, wait)

    for d in near:
        arrive(d)

    lane128 = iota((1, LANES), 1)
    for which in range(2):
        spare = iota((16, WIDE), 0) == 0
        scratch_mid[which][0][9 * 16 :, :] = jnp.where(spare, 1.0, 0.0).astype(BF16)

    def inside_mid(j):
        row = lane128 // COLS + 4 * j + 8 * (r - REACH)
        return (row >= 0) & (row < 8 * ROWS)

    def unpacked(g):
        rows = []
        for k in range(3):
            tile = None
            for j in range(4):
                at = 4 * g + j
                part = own_rows[at - 16] if 16 <= at < 24 else arrived[at].astype(F32)
                part = turned(part, COLS * (k - j))
                tile = part if tile is None else jnp.where(group == j, part, tile)
            rows.append(tile)
        return jnp.concatenate(rows, axis=0)

    steps = []
    for s in range(STEPS2):
        first, last = (0, WIDE // LANES) if s == 0 else (1, WIDE // LANES - 1)
        steps.append(
            Step(
                first, last, COLS, 12, inside_mid, mix2.at[s],
                w1_mid.at[s], w2_mid.at[s], b2_mid.at[s], w3_mid.at[s], bias2.at[s], scratch_mid[s % 2], parts=MID_PARTS,
            )
        )
    states = [{} for _ in range(STEPS2 + 1)]
    own = (4, 5)
    loglik_terms = []

    def finish(s, j):
        step = steps[s]
        u, out = step.u[j], step.out(j)
        sigmoid, log_sigmoid = gate(out[:16])
        if j in own:
            loglik_terms.append(log_sigmoid)
        mixed = (u[8:16] + out[8:16]) * pltpu.roll(sigmoid[8:16], 4, 0)
        mixed = jnp.where(iota((8, 1), 0) < 4, u[8:16], mixed)
        rest = (u[16:24] + out[16:24]) * sigmoid[:8]
        states[s + 1][j] = jnp.concatenate([u[:8], mixed, rest, ones_block(LANES, 8, 0)], axis=0)

    for s, part, t in ORDER:
        step = steps[s]
        if part == 0:
            if s == 0:
                step.take(t, [unpacked(j) for j in step.pair(t)])
            else:
                step.mix(t, lambda j: states[s][j])
        elif part == 1:
            step.patch(t)
        elif part == 2:
            step.one(t)
        elif part == 3:
            step.two(t)
        elif part == 4:
            step.three(t)
        else:
            for j in step.pair(t):
                if s == STEPS2 - 1 or 1 <= j < WIDE // LANES - 1:
                    finish(s, j)

    final = states[STEPS2]
    for half in range(2):
        latent = final[own[half]][:16]
        loglik_terms.append(-0.5 * latent * latent)
        sent_latent[half] = latent
    loglik_sum = jnp.where(iota((16, LANES), 0) < 12, sum(loglik_terms), 0.0)

    lane, to = iota((2 * LANES, 2 * LANES), 0), iota((2 * LANES, 2 * LANES), 1)
    p, col = lane // COLS, lane % COLS
    place = (2 * (p % 2) + col % 2) * 64 + (p // 2) * 16 + col // 2
    permutation = jnp.where(place == to, 1.0, 0.0).astype(BF16)
    streams = []
    for block in range(3):
        pair = [final[2 + 2 * block], final[3 + 2 * block]]
        rest = jnp.concatenate([jnp.concatenate([x[16:24], x[8:16]], axis=0) for x in pair], axis=1)
        for _ in range(2):
            high = rest.astype(BF16)
            streams.append(high)
            rest = rest - high.astype(F32)
    apart = dot(jnp.concatenate(streams, axis=0), permutation)
    blocks = [
        apart[32 * b : 32 * b + 16] + apart[32 * b + 16 : 32 * b + 32]
        for b in range(3)
    ]
    squeezed = []
    for ij in range(4):
        half, sub = LANES * (ij // 2), 64 * (ij % 2)
        rows0, rows4, rows8 = (b[:, half : half + LANES] for b in blocks)
        left = jnp.where(lane128 < 32, turned(rows0, sub + 32), turned(rows4, sub - 32))
        left = jnp.where(lane128 < 96, left, turned(rows8, sub - 96))
        right = jnp.where(lane128 < 96, turned(rows8, sub + 32), turned(rows0, sub - 96))
        squeezed.append(jnp.concatenate([left, right], axis=1))
    state = jnp.concatenate(squeezed + [ones_block(NTOP, 16, 0)], axis=0)

    def latent_copy(k):
        to = lax.rem(c + k, CHAN)
        return pltpu.make_async_remote_copy(
            src_ref=sent_latent.at[to // 4],
            dst_ref=got_latent.at[c],
            send_sem=latent_send,
            recv_sem=latent_recv,
            device_id={"chan": to},
            device_id_type=MESH,
        )

    for k in range(1, CHAN):
        latent_copy(k).start()
    got_latent[c] = sent_latent[c // 4]

    def inside_top(j):
        row = (lane128 // 16 + 8 * j + 2) % 16
        return (row + 4 * r >= 4) & (row + 4 * r < 4 * ROWS + 4) & (row < 12)

    own_top = (lane128 >= 32) & (lane128 < 96)
    top_terms = jnp.zeros((24, LANES), F32)
    for s in range(STEPS3):
        step = Step(
            0, 2 - s, 16, 24, inside_top, mix3.at[s],
            w1_top.at[s], w2_top.at[s], b2_top.at[s], w3_top.at[s], bias3.at[s], scratch_top,
            per=2 - s, wrap=None if s else 2, parts=TOP_PARTS,
        )
        step.mix(0, lambda j: state[:, LANES * j : LANES * (j + 1)])
        step.patch(0)
        step.one(0)
        step.two(0)
        step.three(0)
        u, out = step.u[0], step.out(0)
        sigmoid, log_sigmoid = gate(out[:24])
        top_terms += log_sigmoid
        state = jnp.concatenate([u[:24], (u[24:] + out[24:]) * sigmoid, ones_block(LANES, 32, 0)], axis=0)
    z = state[:C3, :LANES]
    squares = z * z
    top_terms = jnp.where(own_top, top_terms - 0.5 * (squares[:24] + squares[24:]), 0.0)

    logdets = 256.0 * (jnp.sum(small2[1][...]) + jnp.sum(small2[4][...]))
    logdets += 64.0 * (jnp.sum(small3[1][...]) + jnp.sum(small3[4][...]))
    total = jnp.sum(loglik_sum) + jnp.sum(top_terms) + logdets
    total = (total - 0.5 * LOG_TWO_PI * (12 * 256 + 48 * 64)) * (1.0 / DIMS)
    terms[r] = jnp.full((1, LANES), total, F32)

    def term_copy(k):
        return pltpu.make_async_remote_copy(
            src_ref=terms.at[r],
            dst_ref=terms.at[r],
            send_sem=term_send,
            recv_sem=term_recv,
            device_id={"rows": (r + k) % ROWS},
            device_id_type=MESH,
        )

    for k in (4, 3, 5, 2, 6, 1, 7):
        term_copy(k).start()

    latent_top[0] = z.T[32:96].reshape(4, 16, C3)

    others = got_latent.at[pl.ds(0, CHAN - 1)]
    pltpu.make_async_copy(others, others, latent_recv).wait()
    for i in range(8):
        lined = pltpu.roll(got_latent[i], (LANES - COLS * (c % 4)) % LANES, 1)
        latent_mid[12 * i : 12 * i + 12, :] = lined[:12, :COLS]

    others = terms.at[pl.ds(0, ROWS - 1)]
    pltpu.make_async_copy(others, others, term_recv).wait()
    whole = terms[0]
    for i in range(1, ROWS):
        whole = whole + terms[i]
    loglik[...] = whole

    pltpu.make_async_copy(others, others, term_send).wait()
    others = got_latent.at[pl.ds(0, CHAN - 1)]
    pltpu.make_async_copy(others, others, latent_send).wait()
    for d in near:

        def left_here(d=d):
            tiles = packed_half if d else packed.at[pl.ds(0, CHAN - 1)]
            pltpu.make_async_copy(tiles, tiles, send_sem).wait()

        sends(d, left_here)


def leave(latent_mid, latent_top, loglik, latent_mid_out, latent_top_out, loglik_out, sem):
    copies = [
        pltpu.make_async_copy(src, dst, sem.at[i])
        for i, (src, dst) in enumerate(
            ((latent_mid, latent_mid_out), (latent_top, latent_top_out), (loglik, loglik_out))
        )
    ]
    for copy in copies:
        copy.start()
    for copy in copies:
        copy.wait()


def body(*given):
    given = list(given)
    given[0] = given[0].reshape(8, C2, COLS)
    given[10] = given[10].transpose(0, 1, 3, 2)
    given[21] = given[21].transpose(0, 1, 3, 2)

    def small(n, steps):
        return (
            pltpu.VMEM((steps, n), F32),
            pltpu.VMEM((steps, n), F32),
            pltpu.VMEM((steps, n, n), F32),
            pltpu.VMEM((steps, n, n), F32),
            pltpu.VMEM((steps, n), F32),
            pltpu.VMEM((steps, HID), BF16),
            pltpu.VMEM((steps, HID), F32),
            pltpu.VMEM((steps, n), F32),
        )

    def inner(taps, lanes, outs):
        return (
            pltpu.VMEM((taps, lanes), BF16),
            pltpu.VMEM((HID, lanes), BF16),
            pltpu.VMEM((HID, lanes), BF16),
            pltpu.VMEM((9 * outs, lanes), F32),
        )

    latent_mid, latent_top, loglik = pl.pallas_call(
        kernel,
        out_shape=(
            pltpu.VMEM((8 * 12, COLS), F32),
            pltpu.VMEM((1, 4, 16, C3), F32),
            pltpu.VMEM((1, LANES), F32),
        ),
        in_specs=[pl.BlockSpec(memory_space=pl.ANY)] * 23,
        out_specs=tuple(pl.BlockSpec(memory_space=pltpu.VMEM) for _ in range(3)),
        scratch_shapes=[
            pltpu.VMEM((8, C2, COLS), F32),
            pltpu.VMEM((8, 8, LANES), F32),
            pltpu.VMEM((8, 8, LANES), BF16),
            pltpu.VMEM((8 * BLOCKS, 8, LANES), BF16),
            pltpu.VMEM((8, 8, LANES), F32),
            pltpu.VMEM((STEPS2, 9, 12, HID), BF16),
            pltpu.VMEM((STEPS2, HID, HID), BF16),
            pltpu.VMEM((STEPS2, 9, C2, HID), BF16),
            pltpu.VMEM((STEPS3, 9, 24, HID), BF16),
            pltpu.VMEM((STEPS3, HID, HID), BF16),
            pltpu.VMEM((STEPS3, 9, C3, HID), BF16),
            small(C2, STEPS2),
            small(C3, STEPS3),
            pltpu.VMEM((STEPS2, C2, 96), BF16),
            pltpu.VMEM((STEPS3, C3, 240), BF16),
            pltpu.VMEM((STEPS2, C2, 1), F32),
            pltpu.VMEM((STEPS3, C3, 1), F32),
            pltpu.VMEM((KTOP, HID), F32),
            pltpu.VMEM((STEPS2, HID, KMID), BF16),
            pltpu.VMEM((STEPS2, HID, HID), BF16),
            pltpu.VMEM((STEPS2, HID, LANES), F32),
            pltpu.VMEM((STEPS2, 9 * C2, HID), BF16),
            pltpu.VMEM((STEPS3, HID, KTOP), BF16),
            pltpu.VMEM((STEPS3, HID, HID), BF16),
            pltpu.VMEM((STEPS3, HID, LANES), F32),
            pltpu.VMEM((STEPS3, 9 * C3, HID), BF16),
            pltpu.VMEM((2, 16, LANES), F32),
            pltpu.VMEM((CHAN, 16, LANES), F32),
            pltpu.VMEM((ROWS, 1, LANES), F32),
            tuple(inner(KMID, WIDE, C2) for _ in range(2)),
            inner(KTOP, NTOP, C3),
            pltpu.SemaphoreType.DMA,
            pltpu.SemaphoreType.DMA((16,)),
            pltpu.SemaphoreType.DMA((15,)),
            pltpu.SemaphoreType.DMA,
            pltpu.SemaphoreType.DMA((BLOCKS,)),
            pltpu.SemaphoreType.DMA,
            pltpu.SemaphoreType.DMA,
            pltpu.SemaphoreType.DMA,
            pltpu.SemaphoreType.DMA,
        ],
        compiler_params=pltpu.CompilerParams(collective_id=0, has_side_effects=True, vmem_limit_bytes=60 * 2**20),
    )(*given)
    latent_mid, latent_top, loglik = pl.pallas_call(
        leave,
        out_shape=(
            jax.ShapeDtypeStruct((8 * 12, COLS), F32),
            jax.ShapeDtypeStruct((1, 4, 16, C3), F32),
            jax.ShapeDtypeStruct((1, LANES), F32),
        ),
        in_specs=[pl.BlockSpec(memory_space=pltpu.VMEM)] * 3,
        out_specs=tuple(pl.BlockSpec(memory_space=pl.ANY) for _ in range(3)),
        scratch_shapes=[pltpu.SemaphoreType.DMA((3,))],
    )(*(pltpu.with_memory_space_constraint(x, pltpu.VMEM) for x in (latent_mid, latent_top, loglik)))
    return (
        latent_mid.reshape(8, 12, 1, COLS),
        latent_top.transpose(0, 3, 1, 2),
        loglik[0, :1],
    )


def solution(mesh):
    placed = (P("batch", None, ("rows", "chan"), None),) + (P(),) * 22
    return jax.shard_map(
        body,
        mesh=mesh,
        in_specs=placed,
        out_specs=(
            P("batch", None, ("rows", "chan"), None),
            P(("batch", "chan"), None, "rows", None),
            P(("batch", "chan")),
        ),
        check_vma=False,
    )
```

```python
import math

import jax
import jax.numpy as jnp
from jax import lax
from jax.experimental import pallas as pl
from jax.experimental.pallas import tpu as pltpu
from jax.sharding import PartitionSpec as P

MESH = pl.DeviceIdType.MESH
F32 = jnp.float32
BF16 = jnp.bfloat16
LOG_TWO_PI = math.log(2.0 * math.pi)

HID = 512
ROWS = 8
CHAN = 8
C2, C3 = 24, 48
STEPS2, STEPS3 = 3, 2
COLS = 32
LANES = 128
REACH = 2
BLOCKS = 2 * REACH + 1
WIDE = BLOCKS * 8 * COLS
NARROW = WIDE - 2 * LANES
KMID = 160
KTOP = 224
NTOP = 256
DIMS = 24 * 64 * 32


def iota(shape, dim):
    return lax.broadcasted_iota(jnp.int32, shape, dim)


def dot(a, b):
    return jnp.dot(a, b, preferred_element_type=F32)


def exact_dot(a, b):
    return jnp.dot(a, b, preferred_element_type=F32, precision=lax.Precision.HIGHEST)


def column(row):
    n = row.shape[1]
    eye = iota((n, n), 0) == iota((n, n), 1)
    return jnp.sum(jnp.where(eye, row, 0.0), axis=1, keepdims=True)


def place_mid(n, dim):
    at = iota((n, n), dim)
    return jnp.where(at < 12, at, jnp.where(at < 16, at + 8, at - 4))


def mixing(shift, gain, lower, upper, diag):
    n = shift.shape[1]
    i, j = iota((n, n), 0), iota((n, n), 1)
    low = jnp.where(j < i, lower, 0.0) + jnp.where(i == j, 1.0, 0.0)
    up = jnp.where(j > i, upper, 0.0) + jnp.where(i == j, jnp.exp(diag), 0.0)
    a = exact_dot(low, up) * jnp.exp(gain)
    return a, jnp.sum(a * shift, axis=1, keepdims=True)


def stacked(a, b, width, bias_at):
    rows, n = a.shape
    if width > n:
        a = jnp.concatenate([a, jnp.zeros((rows, width - n), F32)], axis=1)
    a = jnp.where(iota((rows, width), 1) == bias_at, b, a)
    high = a.astype(BF16).astype(F32)
    low = a - high
    return jnp.concatenate([high, high, low], axis=1).astype(BF16)


def split_mix(a, v):
    high = v.astype(BF16)
    low = (v - high.astype(F32)).astype(BF16)
    return dot(a, jnp.concatenate([high, low, high], axis=0))


def roll(x, by):
    n = x.shape[1]
    by = by % n
    return x if by == 0 else pltpu.roll(x, by, 1)


def ones_block(n, height, at):
    return jnp.where(iota((height, n), 0) == at, 1.0, 0.0)


def turned(x, by):
    return pltpu.roll(x, -by % LANES, 1)


def moved(blocks, j, by, lane):
    if by == 0:
        return blocks(j, 0)
    here, beside = blocks(j, by), blocks(j + (1 if by > 0 else -1), by)
    if beside is None:
        return here
    return jnp.where(lane < LANES - by, here, beside) if by > 0 else jnp.where(lane >= -by, here, beside)


def cached(get):
    kept = {}

    def blocks(j, by):
        if (j, by) not in kept:
            x = get(j)
            kept[j, by] = x if x is None or by == 0 else turned(x, by)
        return kept[j, by]

    return blocks


def cut(rows, parts):
    each = -(-rows // parts // 8) * 8
    return [slice(at, min(at + each, rows)) for at in range(0, rows, each)]


class Step:
    def __init__(self, first, last, width, half, inside, mix, w1, w2, b2, w3, b3, scratch, per=2, wrap=None, parts=1):
        self.parts = parts
        self.first, self.last, self.width, self.half, self.per, self.wrap = first, last, width, half, per, wrap
        self.inside, self.mix_w, self.w1, self.w2, self.b2, self.w3, self.b3 = inside, mix, w1, w2, b2, w3, b3
        self.patches, self.h1, self.h2, self.z = scratch
        self.outs = w3.shape[0] // 9
        self.u, self.q = {}, {}
        self.lane = iota((1, LANES), 1)
        col = self.lane % width
        self.edge = {-1: col > 0, 1: col < width - 1}
        self.q_blocks = cached(lambda j: self.q.get(j % wrap if wrap else j))
        self.z_blocks = [
            cached(lambda j, t=t: self.z_block(t, j)) for t in range(9)
        ]

    def pair(self, t):
        return [self.first + self.per * t + i for i in range(self.per)]

    def lanes(self, t):
        return slice(self.per * LANES * t, self.per * LANES * (t + 1))

    def mix(self, blocks, state):
        if len(self.mix_w.shape) == 3:
            n = self.mix_w.shape[0] - 1
            x = [state(j) for j in blocks]
            sums = [[self.mix_w[n]] * len(x), [None] * len(x)]
            for k in range(n):
                weights = self.mix_w[k]
                for i, y in enumerate(x):
                    term, so_far = weights * y[k : k + 1, :], sums[k % 2][i]
                    sums[k % 2][i] = term if so_far is None else so_far + term
            for i, j in enumerate(blocks):
                self.take(j, sums[0][i] + sums[1][i])
            return
        u = split_mix(self.mix_w[...], jnp.concatenate([state(j) for j in blocks], axis=1))
        for i, j in enumerate(blocks):
            self.take(j, u[:, LANES * i : LANES * (i + 1)])

    def take(self, j, u):
        rows = 16 if self.half == 12 else 24
        self.u[j] = u
        self.q[j] = jnp.where(self.inside(j), u[:rows], 0.0)
        if rows == 16:
            self.q[j] = self.q[j].astype(BF16)

    def patch(self, t):
        taps = []
        for dy in (-1, 0, 1):
            for dx in (-1, 0, 1):
                parts = []
                for j in self.pair(t):
                    part = moved(self.q_blocks, j, self.width * dy + dx, self.lane)
                    parts.append(jnp.where(self.edge[dx], part, jnp.zeros_like(part)) if dx else part)
                taps.append(jnp.concatenate(parts, axis=1))
        if self.half == 12:
            for i, tap in enumerate(taps):
                self.patches[16 * i : 16 * (i + 1), self.lanes(t)] = tap
        else:
            taps.append(ones_block(self.per * LANES, 8, 0))
            self.patches[:, self.lanes(t)] = jnp.concatenate(taps, axis=0).astype(BF16)

    def one(self, t):
        patches = self.patches[:, self.lanes(t)]
        for m in cut(HID, self.parts):
            self.h1[m, self.lanes(t)] = jnp.maximum(dot(self.w1[m, :], patches), 0.0).astype(BF16)

    def two(self, t):
        h1 = self.h1[:, self.lanes(t)]
        for m in cut(HID, self.parts):
            bias = jnp.concatenate([self.b2[m, :]] * self.per, axis=1)
            self.h2[m, self.lanes(t)] = jnp.maximum(dot(self.w2[m, :], h1) + bias, 0.0).astype(BF16)

    def three(self, t):
        inside = jnp.concatenate([self.inside(j) for j in self.pair(t)], axis=1)
        h2 = self.h2[:, self.lanes(t)]
        for m in cut(9 * self.outs, self.parts):
            self.z[m, self.lanes(t)] = jnp.where(inside, dot(self.w3[m, :], h2), 0.0)

    def z_block(self, tap, j):
        if self.wrap:
            j = j % self.wrap
        if not self.first <= j < self.last:
            return None
        at = LANES * (j - self.first)
        return self.z[self.outs * tap : self.outs * (tap + 1), at : at + LANES]

    def out(self, j):
        total = self.b3[...]
        for dx in (0, -1, 1):
            side = None
            for dy in (-1, 0, 1):
                part = moved(self.z_blocks[3 * (dy + 1) + dx + 1], j, self.width * dy + dx, self.lane)
                side = part if side is None else side + part
            total = total + (jnp.where(self.edge[dx], side, 0.0) if dx else side)
        return total


def gate(g):
    small = jnp.exp(-jnp.abs(g))
    sigmoid = jnp.where(g >= 0.0, 1.0, small) / (1.0 + small)
    return sigmoid, jnp.minimum(g, 0.0) - jnp.log(1.0 + small)


def emission(windows):
    slots, done = [], {}
    for s, (first, last) in enumerate(windows):
        blocks, tiles = range(first, last), range((last - first) // 2)
        at = {}
        for j in blocks:
            at[0, j] = done[j] if s else (j - first) // 2
        end = -1
        for t in tiles:
            seen = [j for j in range(first + 2 * t - 1, first + 2 * t + 3) if j in blocks]
            at[1, t] = max(at[0, j] for j in seen) + 1
            at[2, t] = end = max(at[1, t], end + 1)
            at[3, t] = at[2, t] + LAG
            at[4, t] = at[2, t] + 2 * LAG
        for j in blocks:
            at[5, j] = max(at[4, (x - first) // 2] for x in (j - 1, j, j + 1) if x in blocks) + 1
            done[j] = at[5, j]
        slots += [(slot, s, part, x) for (part, x), slot in at.items()]
    return [(s, part, x) for _, s, part, x in sorted(slots)]


LAG = 1
MID_PARTS = 2
TOP_PARTS = 4
ORDER = emission(((0, 10), (1, 9), (1, 9)))


def kernel(
    images,
    shift_mid,
    gain_mid,
    lower_mid,
    upper_mid,
    diag_mid,
    first_mid,
    first_bias_mid,
    second_mid,
    second_bias_mid,
    third_mid,
    third_bias_mid,
    shift_top,
    gain_top,
    lower_top,
    upper_top,
    diag_top,
    first_top,
    first_bias_top,
    second_top,
    second_bias_top,
    third_top,
    third_bias_top,
    latent_mid,
    latent_top,
    loglik,
    pictures,
    packed,
    packed_half,
    arrived,
    own_rows,
    first2,
    second2,
    third2,
    first3,
    second3,
    third3,
    small2,
    small3,
    mix2,
    wide2,
    mix3,
    wide3,
    bias2,
    bias3,
    tall,
    w1_mid,
    w2_mid,
    b2_mid,
    w3_mid,
    w1_top,
    w2_top,
    b2_top,
    w3_top,
    sent_latent,
    got_latent,
    terms,
    base,
    scratch_mid,
    scratch_top,
    load_sem,
    small_sem,
    weight_sem,
    send_sem,
    recv_sem,
    latent_send,
    latent_recv,
    term_send,
    term_recv,
):
    r, c = lax.axis_index("rows"), lax.axis_index("chan")
    barrier = pltpu.get_barrier_semaphore()

    picture_load = pltpu.make_async_copy(images, pictures, load_sem)
    picture_load.start()
    given2 = (shift_mid, gain_mid, lower_mid, upper_mid, diag_mid, first_bias_mid, second_bias_mid, third_bias_mid)
    given3 = (shift_top, gain_top, lower_top, upper_top, diag_top, first_bias_top, second_bias_top, third_bias_top)
    small_loads = [
        pltpu.make_async_copy(src, dst, small_sem.at[i])
        for i, (src, dst) in enumerate(zip(given2 + given3, small2 + small3))
    ]
    for load in small_loads:
        load.start()
    weight_loads = []
    for s in range(STEPS2):
        for src, dst in ((second_mid, second2), (first_mid, first2), (third_mid, third2)):
            weight_loads.append(
                pltpu.make_async_copy(src.at[s], dst.at[s], weight_sem.at[len(weight_loads)])
            )
    for s in range(STEPS3):
        for src, dst in ((second_top, second3), (first_top, first3), (third_top, third3)):
            weight_loads.append(
                pltpu.make_async_copy(src.at[s], dst.at[s], weight_sem.at[len(weight_loads)])
            )
    def in_image(d, body):
        if d == 0:
            body()
        else:
            pl.when((r + d >= 0) & (r + d < ROWS))(body)

    near = range(-REACH, REACH + 1)

    arrived[...] = jnp.zeros_like(arrived)
    def greet(d):
        for to in range(CHAN):

            def signal(to=to):
                pl.semaphore_signal(barrier, 1, device_id={"rows": r + d, "chan": to}, device_id_type=MESH)

            if d == 0:
                pl.when(c != to)(signal)
            else:
                signal()

    def greet_far(d):
        pl.semaphore_signal(barrier, 1, device_id={"rows": r + d}, device_id_type=MESH)

    for d in sorted(range(1 - ROWS, ROWS), key=lambda d: (abs(d) > REACH, -abs(d))):
        in_image(d, lambda d=d: greet(d) if abs(d) <= REACH else greet_far(d))

    picture_load.wait()
    def prepare_mix(s):
        shift, gain, lower, upper, diag, _, second_b, third_b = small2
        a, b = mixing(shift[s : s + 1], gain[s : s + 1], lower[s], upper[s], diag[s : s + 1])
        to_rows = jnp.where(place_mid(C2, 0) == iota((C2, C2), 1), 1.0, 0.0)
        a, b = exact_dot(to_rows, a), exact_dot(to_rows, b)
        if s:
            to_columns = jnp.where(place_mid(C2, 1) == iota((C2, C2), 0), 1.0, 0.0)
            a = exact_dot(a, to_columns)
        if s == 0:
            mix2[...] = stacked(a, b, 32, C2)
        else:
            for k in range(C2):
                wide2[s - 1, k] = jnp.broadcast_to(a[:, k : k + 1], (C2, LANES))
            wide2[s - 1, C2] = jnp.broadcast_to(b, (C2, LANES))
        extra = third_b[s : s + 1] + jnp.where(iota((1, C2), 1) < C2 // 2, 2.0, 0.0)
        bias2[s] = jnp.sum(to_rows * extra, axis=1, keepdims=True)

    def prepare_small():
        for s in range(STEPS2):
            if s:
                prepare_mix(s)
            b2_mid[s] = jnp.broadcast_to(small2[6][s : s + 1], (LANES, HID)).T
        shift, gain, lower, upper, diag, _, second_b, third_b = small3
        for s in range(STEPS3):
            a, b = mixing(shift[s : s + 1], gain[s : s + 1], lower[s], upper[s], diag[s : s + 1])
            if s == 0:
                n, k = iota((C3, 64), 0), iota((C3, 64), 1)
                row = n // 4
                at = (n % 4) * 16 + jnp.where(row < 8, row, row + 4)
                a = exact_dot(a, jnp.where(at == k, 1.0, 0.0))
                mix3[...] = stacked(a, b, 80, 64)
            else:
                for k in range(C3):
                    wide3[k] = jnp.broadcast_to(a[:, k : k + 1], (C3, LANES))
                wide3[C3] = jnp.broadcast_to(b, (C3, LANES))
            extra = third_b[s : s + 1] + jnp.where(iota((1, C3), 1) < C3 // 2, 2.0, 0.0)
            bias3[s] = column(extra)
            b2_top[s] = jnp.broadcast_to(second_b[s : s + 1], (LANES, HID)).T

        logdets = 256.0 * (jnp.sum(small2[1][...]) + jnp.sum(small2[4][...]))
        logdets += 64.0 * (jnp.sum(small3[1][...]) + jnp.sum(small3[4][...]))
        logdets -= 0.5 * LOG_TWO_PI * (12 * 256 + 48 * 64)
        corner = (iota((8, LANES), 0) == 0) & (iota((8, LANES), 1) == 0)
        base[...] = jnp.where(corner, logdets, 0.0)

    def prepare_mid(s):
        for i in range(3):
            weight_loads[3 * s + i].wait()
        w2_mid[s] = second2[s].T
        tall[...] = jnp.zeros_like(tall)
        for t in range(9):
            tall[16 * t : 16 * t + 12, :] = first2[s, t].astype(F32)
        tall[144:145, :] = small2[5][s : s + 1].astype(F32)
        w1_mid[s] = tall[:KMID, :].T.astype(BF16)
        to_rows = jnp.where(place_mid(C2, 0) == iota((C2, C2), 1), 1.0, 0.0).astype(BF16)
        for t in range(9):
            w3_mid[s, C2 * t : C2 * (t + 1), :] = dot(to_rows, third2[s, t]).astype(BF16)

    def prepare_top(s):
        for i in range(3):
            weight_loads[3 * STEPS2 + 3 * s + i].wait()
        w2_top[s] = second3[s].T
        for t in range(9):
            tall[24 * t : 24 * (t + 1), :] = first3[s, t].astype(F32)
            w3_top[s, C3 * t : C3 * (t + 1), :] = third3[s, t]
        tall[216:217, :] = small3[5][s : s + 1].astype(F32)
        tall[217:, :] = jnp.zeros((KTOP - 217, HID), F32)
        w1_top[s] = tall[...].T.astype(BF16)

    for load in small_loads:
        load.wait()
    for load in weight_loads:
        load.start()
    prepare_mix(0)
    group = iota((8, LANES), 1) // COLS
    pictures_in = []
    for half in range(2):
        rows = []
        for k in range(3):
            tile = None
            for j in range(4):
                part = pictures[4 * half + j, 8 * k : 8 * k + 8, :]
                part = jnp.concatenate([part, jnp.zeros((8, LANES - COLS), F32)], axis=1)
                part = turned(part, -COLS * j)
                tile = part if tile is None else jnp.where(group == j, part, tile)
            rows.append(tile)
        pictures_in.append(jnp.concatenate(rows + [ones_block(LANES, 8, 0)], axis=0))
    mixed_in = split_mix(mix2[...], jnp.concatenate(pictures_in, axis=1))

    for i in range(8):
        tile = jnp.zeros((8, LANES), F32)
        for k in range(3):
            part = mixed_in[8 * k : 8 * k + 8, LANES * (i // 4) : LANES * (i // 4 + 1)]
            tile = jnp.where(group == k, turned(part, COLS * (i % 4 - k)), tile)
        packed[i] = tile
        packed_half[i] = tile.astype(BF16)

    for edge in range(REACH + 1):
        blocks = REACH + 1 + edge

        def meet(blocks=blocks):
            pl.semaphore_wait(barrier, CHAN * blocks - 1 + ROWS - blocks)

        if edge < REACH:
            pl.when((r == edge) | (r == ROWS - 1 - edge))(meet)
        else:
            pl.when((r >= edge) & (r <= ROWS - 1 - edge))(meet)

    def row_copy(d, k):
        to = lax.rem(c + k, CHAN)
        return pltpu.make_async_remote_copy(
            src_ref=packed_half.at[to] if d else packed.at[to],
            dst_ref=arrived.at[8 * (REACH - d) + c] if d else own_rows.at[c],
            send_sem=send_sem,
            recv_sem=recv_sem.at[REACH - d],
            device_id={"rows": r + d, "chan": to},
            device_id_type=MESH,
        )

    def sends(d, body):
        if d == REACH:
            pl.when((r + d < ROWS) & (c >= 2))(body)
        elif d == -REACH:
            pl.when((r + d >= 0) & (c < CHAN - 2))(body)
        else:
            in_image(d, body)

    for d in sorted(near, key=lambda d: -abs(d)):

        def send(d=d):
            for k in (4, 3, 5, 2, 6, 1, 7) + (() if d == 0 else (0,)):
                row_copy(d, k).start()

        sends(d, send)
    own_rows[c] = packed[c]

    prepare_small()
    for s in range(STEPS2):
        prepare_mid(s)
    for s in range(STEPS3):
        prepare_top(s)

    def arrive(d):
        first, last = 8 * (d + REACH), 8 * (d + REACH) + 8
        if d == -REACH:
            first += 2
        elif d == REACH:
            last -= 2
        tiles = arrived.at[pl.ds(first, last - first)] if d else own_rows.at[pl.ds(0, CHAN - 1)]

        def wait():
            pltpu.make_async_copy(tiles, tiles, recv_sem.at[d + REACH]).wait()

        in_image(d, wait)

    for d in near:
        arrive(d)

    lane128 = iota((1, LANES), 1)
    for which in range(2):
        spare = iota((16, WIDE), 0) == 0
        scratch_mid[which][0][9 * 16 :, :] = jnp.where(spare, 1.0, 0.0).astype(BF16)

    def inside_mid(j):
        row = lane128 // COLS + 4 * j + 8 * (r - REACH)
        return (row >= 0) & (row < 8 * ROWS)

    def unpacked(g):
        rows = []
        for k in range(3):
            tile = None
            for j in range(4):
                at = 4 * g + j
                part = own_rows[at - 16] if 16 <= at < 24 else arrived[at].astype(F32)
                part = turned(part, COLS * (k - j))
                tile = part if tile is None else jnp.where(group == j, part, tile)
            rows.append(tile)
        return jnp.concatenate(rows, axis=0)

    steps = []
    for s in range(STEPS2):
        first, last = (0, WIDE // LANES) if s == 0 else (1, WIDE // LANES - 1)
        steps.append(
            Step(
                first, last, COLS, 12, inside_mid, wide2.at[max(s - 1, 0)],
                w1_mid.at[s], w2_mid.at[s], b2_mid.at[s], w3_mid.at[s], bias2.at[s], scratch_mid[s % 2], parts=MID_PARTS,
            )
        )
    states = [{} for _ in range(STEPS2 + 1)]
    own = (4, 5)
    loglik_terms = []

    def finish(s, j):
        step = steps[s]
        u, out = step.u[j], step.out(j)
        sigmoid, log_sigmoid = gate(out[:16])
        if j in own:
            loglik_terms.append(log_sigmoid)
        mixed = (u[8:16] + out[8:16]) * pltpu.roll(sigmoid[8:16], 4, 0)
        mixed = jnp.where(iota((8, 1), 0) < 4, u[8:16], mixed)
        rest = (u[16:24] + out[16:24]) * sigmoid[:8]
        states[s + 1][j] = jnp.concatenate([u[:8], mixed, rest], axis=0)

    for s, part, at in ORDER:
        step = steps[s]
        if part == 0:
            if s == 0:
                step.take(at, unpacked(at))
            else:
                step.mix([at], lambda j: states[s][j])
        elif part == 1:
            step.patch(at)
        elif part == 2:
            step.one(at)
        elif part == 3:
            step.two(at)
        elif part == 4:
            step.three(at)
        elif s == STEPS2 - 1 or 1 <= at < WIDE // LANES - 1:
            finish(s, at)

    final = states[STEPS2]
    for half in range(2):
        latent = final[own[half]][:16]
        loglik_terms.append(-0.5 * latent * latent)
        sent_latent[half] = latent
    loglik_sum = jnp.where(iota((16, LANES), 0) < 12, sum(loglik_terms), 0.0)

    lane, to = iota((2 * LANES, 2 * LANES), 0), iota((2 * LANES, 2 * LANES), 1)
    p, col = lane // COLS, lane % COLS
    place = (2 * (p % 2) + col % 2) * 64 + (p // 2) * 16 + col // 2
    permutation = jnp.where(place == to, 1.0, 0.0).astype(BF16)
    streams = []
    for block in range(3):
        pair = [final[2 + 2 * block], final[3 + 2 * block]]
        rest = jnp.concatenate([jnp.concatenate([x[16:24], x[8:16]], axis=0) for x in pair], axis=1)
        for _ in range(2):
            high = rest.astype(BF16)
            streams.append(high)
            rest = rest - high.astype(F32)
    apart = dot(jnp.concatenate(streams, axis=0), permutation)
    blocks = [
        apart[32 * b : 32 * b + 16] + apart[32 * b + 16 : 32 * b + 32]
        for b in range(3)
    ]
    squeezed = []
    for ij in range(4):
        half, sub = LANES * (ij // 2), 64 * (ij % 2)
        rows0, rows4, rows8 = (b[:, half : half + LANES] for b in blocks)
        left = jnp.where(lane128 < 32, turned(rows0, sub + 32), turned(rows4, sub - 32))
        left = jnp.where(lane128 < 96, left, turned(rows8, sub - 96))
        right = jnp.where(lane128 < 96, turned(rows8, sub + 32), turned(rows0, sub - 96))
        squeezed.append(jnp.concatenate([left, right], axis=1))
    state = jnp.concatenate(squeezed + [ones_block(NTOP, 16, 0)], axis=0)

    def latent_copy(k):
        to = lax.rem(c + k, CHAN)
        return pltpu.make_async_remote_copy(
            src_ref=sent_latent.at[to // 4],
            dst_ref=got_latent.at[c],
            send_sem=latent_send,
            recv_sem=latent_recv,
            device_id={"chan": to},
            device_id_type=MESH,
        )

    for k in range(1, CHAN):
        latent_copy(k).start()
    got_latent[c] = sent_latent[c // 4]

    def inside_top(j):
        row = (lane128 // 16 + 8 * j + 2) % 16
        return (row + 4 * r >= 4) & (row + 4 * r < 4 * ROWS + 4) & (row < 12)

    own_top = (lane128 >= 32) & (lane128 < 96)
    top_terms = jnp.zeros((24, LANES), F32)
    for s in range(STEPS3):
        step = Step(
            0, 2 - s, 16, 24, inside_top, wide3 if s else mix3,
            w1_top.at[s], w2_top.at[s], b2_top.at[s], w3_top.at[s], bias3.at[s], scratch_top,
            per=2 - s, wrap=None if s else 2, parts=TOP_PARTS,
        )
        step.mix(range(2 - s), lambda j: state[:, LANES * j : LANES * (j + 1)])
        step.patch(0)
        step.one(0)
        step.two(0)
        step.three(0)
        u, out = step.u[0], step.out(0)
        sigmoid, log_sigmoid = gate(out[:24])
        top_terms += log_sigmoid
        state = jnp.concatenate([u[:24], (u[24:] + out[24:]) * sigmoid], axis=0)
    z = state
    squares = z * z
    top_terms = jnp.where(own_top, top_terms - 0.5 * (squares[:24] + squares[24:]), 0.0)

    last = top_terms[:8] + top_terms[8:16] + top_terms[16:]
    last += loglik_sum[:8] + loglik_sum[8:] + base[...]
    terms[r] = jnp.sum(last, axis=0, keepdims=True) * (1.0 / DIMS)

    def term_copy(k):
        return pltpu.make_async_remote_copy(
            src_ref=terms.at[r],
            dst_ref=terms.at[r],
            send_sem=term_send,
            recv_sem=term_recv,
            device_id={"rows": (r + k) % ROWS},
            device_id_type=MESH,
        )

    for k in (4, 3, 5, 2, 6, 1, 7):
        term_copy(k).start()

    latent_top[0] = z.T[32:96].reshape(4, 16, C3)

    others = got_latent.at[pl.ds(0, CHAN - 1)]
    pltpu.make_async_copy(others, others, latent_recv).wait()
    for i in range(8):
        lined = pltpu.roll(got_latent[i], (LANES - COLS * (c % 4)) % LANES, 1)
        latent_mid[12 * i : 12 * i + 12, :] = lined[:12, :COLS]

    others = terms.at[pl.ds(0, ROWS - 1)]
    pltpu.make_async_copy(others, others, term_recv).wait()
    whole = terms[0]
    for i in range(1, ROWS):
        whole = whole + terms[i]
    loglik[...] = jnp.broadcast_to(jnp.sum(whole, axis=1, keepdims=True), (1, LANES))

    pltpu.make_async_copy(others, others, term_send).wait()
    others = got_latent.at[pl.ds(0, CHAN - 1)]
    pltpu.make_async_copy(others, others, latent_send).wait()
    for d in near:

        def left_here(d=d):
            tiles = packed_half if d else packed.at[pl.ds(0, CHAN - 1)]
            pltpu.make_async_copy(tiles, tiles, send_sem).wait()

        sends(d, left_here)


def leave(latent_mid, latent_top, loglik, latent_mid_out, latent_top_out, loglik_out, sem):
    copies = [
        pltpu.make_async_copy(src, dst, sem.at[i])
        for i, (src, dst) in enumerate(
            ((latent_mid, latent_mid_out), (latent_top, latent_top_out), (loglik, loglik_out))
        )
    ]
    for copy in copies:
        copy.start()
    for copy in copies:
        copy.wait()


def body(*given):
    given = list(given)
    given[0] = given[0].reshape(8, C2, COLS)
    given[10] = given[10].transpose(0, 1, 3, 2)
    given[21] = given[21].transpose(0, 1, 3, 2)

    def small(n, steps):
        return (
            pltpu.VMEM((steps, n), F32),
            pltpu.VMEM((steps, n), F32),
            pltpu.VMEM((steps, n, n), F32),
            pltpu.VMEM((steps, n, n), F32),
            pltpu.VMEM((steps, n), F32),
            pltpu.VMEM((steps, HID), BF16),
            pltpu.VMEM((steps, HID), F32),
            pltpu.VMEM((steps, n), F32),
        )

    def inner(taps, lanes, outs):
        return (
            pltpu.VMEM((taps, lanes), BF16),
            pltpu.VMEM((HID, lanes), BF16),
            pltpu.VMEM((HID, lanes), BF16),
            pltpu.VMEM((9 * outs, lanes), F32),
        )

    latent_mid, latent_top, loglik = pl.pallas_call(
        kernel,
        out_shape=(
            pltpu.VMEM((8 * 12, COLS), F32),
            pltpu.VMEM((1, 4, 16, C3), F32),
            pltpu.VMEM((1, LANES), F32),
        ),
        in_specs=[pl.BlockSpec(memory_space=pl.ANY)] * 23,
        out_specs=tuple(pl.BlockSpec(memory_space=pltpu.VMEM) for _ in range(3)),
        scratch_shapes=[
            pltpu.VMEM((8, C2, COLS), F32),
            pltpu.VMEM((8, 8, LANES), F32),
            pltpu.VMEM((8, 8, LANES), BF16),
            pltpu.VMEM((8 * BLOCKS, 8, LANES), BF16),
            pltpu.VMEM((8, 8, LANES), F32),
            pltpu.VMEM((STEPS2, 9, 12, HID), BF16),
            pltpu.VMEM((STEPS2, HID, HID), BF16),
            pltpu.VMEM((STEPS2, 9, C2, HID), BF16),
            pltpu.VMEM((STEPS3, 9, 24, HID), BF16),
            pltpu.VMEM((STEPS3, HID, HID), BF16),
            pltpu.VMEM((STEPS3, 9, C3, HID), BF16),
            small(C2, STEPS2),
            small(C3, STEPS3),
            pltpu.VMEM((C2, 96), BF16),
            pltpu.VMEM((STEPS2 - 1, C2 + 1, C2, LANES), F32),
            pltpu.VMEM((C3, 240), BF16),
            pltpu.VMEM((C3 + 1, C3, LANES), F32),
            pltpu.VMEM((STEPS2, C2, 1), F32),
            pltpu.VMEM((STEPS3, C3, 1), F32),
            pltpu.VMEM((KTOP, HID), F32),
            pltpu.VMEM((STEPS2, HID, KMID), BF16),
            pltpu.VMEM((STEPS2, HID, HID), BF16),
            pltpu.VMEM((STEPS2, HID, LANES), F32),
            pltpu.VMEM((STEPS2, 9 * C2, HID), BF16),
            pltpu.VMEM((STEPS3, HID, KTOP), BF16),
            pltpu.VMEM((STEPS3, HID, HID), BF16),
            pltpu.VMEM((STEPS3, HID, LANES), F32),
            pltpu.VMEM((STEPS3, 9 * C3, HID), BF16),
            pltpu.VMEM((2, 16, LANES), F32),
            pltpu.VMEM((CHAN, 16, LANES), F32),
            pltpu.VMEM((ROWS, 1, LANES), F32),
            pltpu.VMEM((8, LANES), F32),
            tuple(inner(KMID, WIDE, C2) for _ in range(2)),
            inner(KTOP, NTOP, C3),
            pltpu.SemaphoreType.DMA,
            pltpu.SemaphoreType.DMA((16,)),
            pltpu.SemaphoreType.DMA((15,)),
            pltpu.SemaphoreType.DMA,
            pltpu.SemaphoreType.DMA((BLOCKS,)),
            pltpu.SemaphoreType.DMA,
            pltpu.SemaphoreType.DMA,
            pltpu.SemaphoreType.DMA,
            pltpu.SemaphoreType.DMA,
        ],
        compiler_params=pltpu.CompilerParams(collective_id=0, has_side_effects=True, vmem_limit_bytes=60 * 2**20),
    )(*given)
    latent_mid, latent_top, loglik = pl.pallas_call(
        leave,
        out_shape=(
            jax.ShapeDtypeStruct((8 * 12, COLS), F32),
            jax.ShapeDtypeStruct((1, 4, 16, C3), F32),
            jax.ShapeDtypeStruct((1, LANES), F32),
        ),
        in_specs=[pl.BlockSpec(memory_space=pltpu.VMEM)] * 3,
        out_specs=tuple(pl.BlockSpec(memory_space=pl.ANY) for _ in range(3)),
        scratch_shapes=[pltpu.SemaphoreType.DMA((3,))],
    )(*(pltpu.with_memory_space_constraint(x, pltpu.VMEM) for x in (latent_mid, latent_top, loglik)))
    return (
        latent_mid.reshape(8, 12, 1, COLS),
        latent_top.transpose(0, 3, 1, 2),
        loglik[0, :1],
    )


def solution(mesh):
    placed = (P("batch", None, ("rows", "chan"), None),) + (P(),) * 22
    return jax.shard_map(
        body,
        mesh=mesh,
        in_specs=placed,
        out_specs=(
            P("batch", None, ("rows", "chan"), None),
            P(("batch", "chan"), None, "rows", None),
            P(("batch", "chan")),
        ),
        check_vma=False,
    )
```

```python
import math

import jax
import jax.numpy as jnp
from jax import lax
from jax.experimental import pallas as pl
from jax.experimental.pallas import tpu as pltpu
from jax.sharding import PartitionSpec as P

MESH = pl.DeviceIdType.MESH
F32 = jnp.float32
BF16 = jnp.bfloat16
LOG_TWO_PI = math.log(2.0 * math.pi)

HID = 512
ROWS = 8
CHAN = 8
C2, C3 = 24, 48
STEPS2, STEPS3 = 3, 2
COLS = 32
LANES = 128
REACH = 2
BLOCKS = 2 * REACH + 1
WIDE = BLOCKS * 8 * COLS
NARROW = WIDE - 2 * LANES
KMID = 160
KTOP = 224
NTOP = 256
DIMS = 24 * 64 * 32


def iota(shape, dim):
    return lax.broadcasted_iota(jnp.int32, shape, dim)


def dot(a, b):
    return jnp.dot(a, b, preferred_element_type=F32)


def exact_dot(a, b):
    return jnp.dot(a, b, preferred_element_type=F32, precision=lax.Precision.HIGHEST)


def column(row):
    n = row.shape[1]
    eye = iota((n, n), 0) == iota((n, n), 1)
    return jnp.sum(jnp.where(eye, row, 0.0), axis=1, keepdims=True)


def place_mid(n, dim):
    at = iota((n, n), dim)
    return jnp.where(at < 12, at, jnp.where(at < 16, at + 8, at - 4))


def mixing(shift, gain, lower, upper, diag):
    n = shift.shape[1]
    i, j = iota((n, n), 0), iota((n, n), 1)
    low = jnp.where(j < i, lower, 0.0) + jnp.where(i == j, 1.0, 0.0)
    up = jnp.where(j > i, upper, 0.0) + jnp.where(i == j, jnp.exp(diag), 0.0)
    a = exact_dot(low, up) * jnp.exp(gain)
    return a, jnp.sum(a * shift, axis=1, keepdims=True)


def stacked(a, b, width, bias_at):
    rows, n = a.shape
    if width > n:
        a = jnp.concatenate([a, jnp.zeros((rows, width - n), F32)], axis=1)
    a = jnp.where(iota((rows, width), 1) == bias_at, b, a)
    high = a.astype(BF16).astype(F32)
    low = a - high
    return jnp.concatenate([high, high, low], axis=1).astype(BF16)


def split_mix(a, v):
    high = v.astype(BF16)
    low = (v - high.astype(F32)).astype(BF16)
    return dot(a, jnp.concatenate([high, low, high], axis=0))


def roll(x, by):
    n = x.shape[1]
    by = by % n
    return x if by == 0 else pltpu.roll(x, by, 1)


def ones_block(n, height, at):
    return jnp.where(iota((height, n), 0) == at, 1.0, 0.0)


def turned(x, by):
    return pltpu.roll(x, -by % LANES, 1)


def moved(blocks, j, by, lane):
    if by == 0:
        return blocks(j, 0)
    here, beside = blocks(j, by), blocks(j + (1 if by > 0 else -1), by)
    if beside is None:
        return here
    return jnp.where(lane < LANES - by, here, beside) if by > 0 else jnp.where(lane >= -by, here, beside)


def cached(get):
    kept = {}

    def blocks(j, by):
        if (j, by) not in kept:
            x = get(j)
            kept[j, by] = x if x is None or by == 0 else turned(x, by)
        return kept[j, by]

    return blocks


def cut(rows, parts):
    each = -(-rows // parts // 8) * 8
    return [slice(at, min(at + each, rows)) for at in range(0, rows, each)]


class Step:
    def __init__(self, first, last, width, half, inside, mix, w1, w2, b2, w3, b3, scratch, per=2, wrap=None, parts=1):
        self.parts = parts
        self.first, self.last, self.width, self.half, self.per, self.wrap = first, last, width, half, per, wrap
        self.inside, self.mix_w, self.w1, self.w2, self.b2, self.w3, self.b3 = inside, mix, w1, w2, b2, w3, b3
        self.patches, self.h1, self.h2, self.z = scratch
        self.outs = w3.shape[0] // 9
        self.u, self.q = {}, {}
        self.lane = iota((1, LANES), 1)
        col = self.lane % width
        self.edge = {-1: col > 0, 1: col < width - 1}
        self.q_blocks = cached(lambda j: self.q.get(j % wrap if wrap else j))
        self.z_blocks = [
            cached(lambda j, t=t: self.z_block(t, j)) for t in range(9)
        ]

    def pair(self, t):
        return [self.first + self.per * t + i for i in range(self.per)]

    def lanes(self, t):
        return slice(self.per * LANES * t, self.per * LANES * (t + 1))

    def mix(self, blocks, state):
        if len(self.mix_w.shape) == 3:
            n = self.mix_w.shape[0] - 1
            x = [state(j) for j in blocks]
            sums = [[self.mix_w[n]] * len(x), [None] * len(x)]
            for k in range(n):
                weights = self.mix_w[k]
                for i, y in enumerate(x):
                    term, so_far = weights * y[k : k + 1, :], sums[k % 2][i]
                    sums[k % 2][i] = term if so_far is None else so_far + term
            for i, j in enumerate(blocks):
                self.take(j, sums[0][i] + sums[1][i])
            return
        u = split_mix(self.mix_w[...], jnp.concatenate([state(j) for j in blocks], axis=1))
        for i, j in enumerate(blocks):
            self.take(j, u[:, LANES * i : LANES * (i + 1)])

    def take(self, j, u):
        rows = 16 if self.half == 12 else 24
        self.u[j] = u
        self.q[j] = jnp.where(self.inside(j), u[:rows], 0.0)
        if rows == 16:
            self.q[j] = self.q[j].astype(BF16)

    def patch(self, t):
        taps = []
        for dy in (-1, 0, 1):
            for dx in (-1, 0, 1):
                parts = []
                for j in self.pair(t):
                    part = moved(self.q_blocks, j, self.width * dy + dx, self.lane)
                    parts.append(jnp.where(self.edge[dx], part, jnp.zeros_like(part)) if dx else part)
                taps.append(jnp.concatenate(parts, axis=1))
        if self.half == 12:
            for i, tap in enumerate(taps):
                self.patches[16 * i : 16 * (i + 1), self.lanes(t)] = tap
        else:
            taps.append(ones_block(self.per * LANES, 8, 0))
            self.patches[:, self.lanes(t)] = jnp.concatenate(taps, axis=0).astype(BF16)

    def one(self, t):
        patches = self.patches[:, self.lanes(t)]
        for m in cut(HID, self.parts):
            self.h1[m, self.lanes(t)] = jnp.maximum(dot(self.w1[m, :], patches), 0.0).astype(BF16)

    def two(self, t):
        h1 = self.h1[:, self.lanes(t)]
        for m in cut(HID, self.parts):
            bias = jnp.concatenate([self.b2[m, :]] * self.per, axis=1)
            self.h2[m, self.lanes(t)] = jnp.maximum(dot(self.w2[m, :], h1) + bias, 0.0).astype(BF16)

    def three(self, t):
        inside = jnp.concatenate([self.inside(j) for j in self.pair(t)], axis=1)
        h2 = self.h2[:, self.lanes(t)]
        for m in cut(9 * self.outs, self.parts):
            self.z[m, self.lanes(t)] = jnp.where(inside, dot(self.w3[m, :], h2), 0.0)

    def z_block(self, tap, j):
        if self.wrap:
            j = j % self.wrap
        if not self.first <= j < self.last:
            return None
        at = LANES * (j - self.first)
        return self.z[self.outs * tap : self.outs * (tap + 1), at : at + LANES]

    def out(self, j):
        total = self.b3[...]
        for dx in (0, -1, 1):
            side = None
            for dy in (-1, 0, 1):
                part = moved(self.z_blocks[3 * (dy + 1) + dx + 1], j, self.width * dy + dx, self.lane)
                side = part if side is None else side + part
            total = total + (jnp.where(self.edge[dx], side, 0.0) if dx else side)
        return total


def gate(g):
    small = jnp.exp(-jnp.abs(g))
    sigmoid = jnp.where(g >= 0.0, 1.0, small) / (1.0 + small)
    return sigmoid, jnp.minimum(g, 0.0) - jnp.log(1.0 + small)


def emission(windows):
    slots, done = [], {}
    for s, (first, last) in enumerate(windows):
        blocks, tiles = range(first, last), range((last - first) // 2)
        at = {}
        for j in blocks:
            at[0, j] = done[j] if s else (j - first) // 2
        end = -1
        for t in tiles:
            seen = [j for j in range(first + 2 * t - 1, first + 2 * t + 3) if j in blocks]
            at[1, t] = max(at[0, j] for j in seen) + 1
            at[2, t] = end = max(at[1, t], end + 1)
            at[3, t] = at[2, t] + LAG
            at[4, t] = at[2, t] + 2 * LAG
        for j in blocks:
            at[5, j] = max(at[4, (x - first) // 2] for x in (j - 1, j, j + 1) if x in blocks) + 1
            done[j] = at[5, j]
        slots += [(slot, s, part, x) for (part, x), slot in at.items()]
    return [(s, part, x) for _, s, part, x in sorted(slots)]


LAG = 1
MID_PARTS = 2
TOP_PARTS = 4
ORDER = emission(((0, 10), (1, 9), (1, 9)))


def kernel(
    images,
    shift_mid,
    gain_mid,
    lower_mid,
    upper_mid,
    diag_mid,
    first_mid,
    first_bias_mid,
    second_mid,
    second_bias_mid,
    third_mid,
    third_bias_mid,
    shift_top,
    gain_top,
    lower_top,
    upper_top,
    diag_top,
    first_top,
    first_bias_top,
    second_top,
    second_bias_top,
    third_top,
    third_bias_top,
    latent_mid,
    latent_top,
    loglik,
    pictures,
    packed,
    packed_half,
    arrived,
    own_rows,
    first2,
    second2,
    third2,
    first3,
    second3,
    third3,
    small2,
    small3,
    mix2,
    wide2,
    mix3,
    wide3,
    bias2,
    bias3,
    tall,
    w1_mid,
    w2_mid,
    b2_mid,
    w3_mid,
    w1_top,
    w2_top,
    b2_top,
    w3_top,
    sent_latent,
    got_latent,
    terms,
    base,
    scratch_mid,
    scratch_top,
    load_sem,
    small_sem,
    weight_sem,
    send_sem,
    recv_sem,
    latent_send,
    latent_recv,
    term_send,
    term_recv,
):
    r, c = lax.axis_index("rows"), lax.axis_index("chan")
    barrier = pltpu.get_barrier_semaphore()

    picture_load = pltpu.make_async_copy(images, pictures, load_sem)
    picture_load.start()
    given2 = (shift_mid, gain_mid, lower_mid, upper_mid, diag_mid, first_bias_mid, second_bias_mid, third_bias_mid)
    given3 = (shift_top, gain_top, lower_top, upper_top, diag_top, first_bias_top, second_bias_top, third_bias_top)
    small_loads = [
        pltpu.make_async_copy(src, dst, small_sem.at[i])
        for i, (src, dst) in enumerate(zip(given2 + given3, small2 + small3))
    ]
    for load in small_loads:
        load.start()
    given_weights = (second_mid, first_mid, third_mid, second_top, first_top, third_top)
    kept_weights = (second2, first2, third2, second3, first3, third3)
    weight_loads = [
        pltpu.make_async_copy(src, dst, weight_sem.at[i])
        for i, (src, dst) in enumerate(zip(given_weights, kept_weights))
    ]

    def in_image(d, body):
        if d == 0:
            body()
        else:
            pl.when((r + d >= 0) & (r + d < ROWS))(body)

    near = range(-REACH, REACH + 1)

    arrived[...] = jnp.zeros_like(arrived)
    def greet(d):
        for to in range(CHAN):

            def signal(to=to):
                pl.semaphore_signal(barrier, 1, device_id={"rows": r + d, "chan": to}, device_id_type=MESH)

            if d == 0:
                pl.when(c != to)(signal)
            else:
                signal()

    def greet_far(d):
        pl.semaphore_signal(barrier, 1, device_id={"rows": r + d}, device_id_type=MESH)

    for d in sorted(range(1 - ROWS, ROWS), key=lambda d: (abs(d) > REACH, -abs(d))):
        in_image(d, lambda d=d: greet(d) if abs(d) <= REACH else greet_far(d))

    picture_load.wait()
    def prepare_mix(s):
        shift, gain, lower, upper, diag, _, second_b, third_b = small2
        a, b = mixing(shift[s : s + 1], gain[s : s + 1], lower[s], upper[s], diag[s : s + 1])
        to_rows = jnp.where(place_mid(C2, 0) == iota((C2, C2), 1), 1.0, 0.0)
        a, b = exact_dot(to_rows, a), exact_dot(to_rows, b)
        if s:
            to_columns = jnp.where(place_mid(C2, 1) == iota((C2, C2), 0), 1.0, 0.0)
            a = exact_dot(a, to_columns)
        if s == 0:
            mix2[...] = stacked(a, b, 32, C2)
        else:
            for k in range(C2):
                wide2[s - 1, k] = jnp.broadcast_to(a[:, k : k + 1], (C2, LANES))
            wide2[s - 1, C2] = jnp.broadcast_to(b, (C2, LANES))
        extra = third_b[s : s + 1] + jnp.where(iota((1, C2), 1) < C2 // 2, 2.0, 0.0)
        bias2[s] = jnp.sum(to_rows * extra, axis=1, keepdims=True)

    def prepare_small():
        for s in range(STEPS2):
            if s:
                prepare_mix(s)
            b2_mid[s] = jnp.broadcast_to(small2[6][s : s + 1], (LANES, HID)).T
        shift, gain, lower, upper, diag, _, second_b, third_b = small3
        for s in range(STEPS3):
            a, b = mixing(shift[s : s + 1], gain[s : s + 1], lower[s], upper[s], diag[s : s + 1])
            if s == 0:
                n, k = iota((C3, 64), 0), iota((C3, 64), 1)
                row = n // 4
                at = (n % 4) * 16 + jnp.where(row < 8, row, row + 4)
                a = exact_dot(a, jnp.where(at == k, 1.0, 0.0))
                mix3[...] = stacked(a, b, 80, 64)
            else:
                for k in range(C3):
                    wide3[k] = jnp.broadcast_to(a[:, k : k + 1], (C3, LANES))
                wide3[C3] = jnp.broadcast_to(b, (C3, LANES))
            extra = third_b[s : s + 1] + jnp.where(iota((1, C3), 1) < C3 // 2, 2.0, 0.0)
            bias3[s] = column(extra)
            b2_top[s] = jnp.broadcast_to(second_b[s : s + 1], (LANES, HID)).T

        logdets = 256.0 * (jnp.sum(small2[1][...]) + jnp.sum(small2[4][...]))
        logdets += 64.0 * (jnp.sum(small3[1][...]) + jnp.sum(small3[4][...]))
        logdets -= 0.5 * LOG_TWO_PI * (12 * 256 + 48 * 64)
        corner = (iota((8, LANES), 0) == 0) & (iota((8, LANES), 1) == 0)
        base[...] = jnp.where(corner, logdets, 0.0)

    def prepare_mid(s):
        if s == 0:
            for load in weight_loads[:3]:
                load.wait()
        w2_mid[s] = second2[s].T
        tall[...] = jnp.zeros_like(tall)
        for t in range(9):
            tall[16 * t : 16 * t + 12, :] = first2[s, t].astype(F32)
        tall[144:145, :] = small2[5][s : s + 1].astype(F32)
        w1_mid[s] = tall[:KMID, :].T.astype(BF16)
        to_rows = jnp.where(place_mid(C2, 0) == iota((C2, C2), 1), 1.0, 0.0).astype(BF16)
        for t in range(9):
            w3_mid[s, C2 * t : C2 * (t + 1), :] = dot(to_rows, third2[s, t]).astype(BF16)

    def prepare_top(s):
        if s == 0:
            for load in weight_loads[3:]:
                load.wait()
        w2_top[s] = second3[s].T
        for t in range(9):
            tall[24 * t : 24 * (t + 1), :] = first3[s, t].astype(F32)
            w3_top[s, C3 * t : C3 * (t + 1), :] = third3[s, t]
        tall[216:217, :] = small3[5][s : s + 1].astype(F32)
        tall[217:, :] = jnp.zeros((KTOP - 217, HID), F32)
        w1_top[s] = tall[...].T.astype(BF16)

    for load in small_loads:
        load.wait()
    for load in weight_loads:
        load.start()
    prepare_mix(0)
    group = iota((8, LANES), 1) // COLS
    pictures_in = []
    for half in range(2):
        rows = []
        for k in range(3):
            tile = None
            for j in range(4):
                part = pictures[4 * half + j, 8 * k : 8 * k + 8, :]
                part = jnp.concatenate([part, jnp.zeros((8, LANES - COLS), F32)], axis=1)
                part = turned(part, -COLS * j)
                tile = part if tile is None else jnp.where(group == j, part, tile)
            rows.append(tile)
        pictures_in.append(jnp.concatenate(rows + [ones_block(LANES, 8, 0)], axis=0))
    mixed_in = split_mix(mix2[...], jnp.concatenate(pictures_in, axis=1))

    for i in range(8):
        tile = jnp.zeros((8, LANES), F32)
        for k in range(3):
            part = mixed_in[8 * k : 8 * k + 8, LANES * (i // 4) : LANES * (i // 4 + 1)]
            tile = jnp.where(group == k, turned(part, COLS * (i % 4 - k)), tile)
        packed[i] = tile
        packed_half[i] = tile.astype(BF16)

    for edge in range(REACH + 1):
        blocks = REACH + 1 + edge

        def meet(blocks=blocks):
            pl.semaphore_wait(barrier, CHAN * blocks - 1 + ROWS - blocks)

        if edge < REACH:
            pl.when((r == edge) | (r == ROWS - 1 - edge))(meet)
        else:
            pl.when((r >= edge) & (r <= ROWS - 1 - edge))(meet)

    def row_copy(d, k):
        to = lax.rem(c + k, CHAN)
        return pltpu.make_async_remote_copy(
            src_ref=packed_half.at[to] if d else packed.at[to],
            dst_ref=arrived.at[8 * (REACH - d) + c] if d else own_rows.at[c],
            send_sem=send_sem,
            recv_sem=recv_sem.at[REACH - d],
            device_id={"rows": r + d, "chan": to},
            device_id_type=MESH,
        )

    def sends(d, body):
        if d == REACH:
            pl.when((r + d < ROWS) & (c >= 2))(body)
        elif d == -REACH:
            pl.when((r + d >= 0) & (c < CHAN - 2))(body)
        else:
            in_image(d, body)

    for d in sorted(near, key=lambda d: -abs(d)):

        def send(d=d):
            for k in (4, 3, 5, 2, 6, 1, 7) + (() if d == 0 else (0,)):
                row_copy(d, k).start()

        sends(d, send)
    own_rows[c] = packed[c]

    prepare_small()
    for s in range(STEPS2):
        prepare_mid(s)
    for s in range(STEPS3):
        prepare_top(s)

    def arrive(d):
        first, last = 8 * (d + REACH), 8 * (d + REACH) + 8
        if d == -REACH:
            first += 2
        elif d == REACH:
            last -= 2
        tiles = arrived.at[pl.ds(first, last - first)] if d else own_rows.at[pl.ds(0, CHAN - 1)]

        def wait():
            pltpu.make_async_copy(tiles, tiles, recv_sem.at[d + REACH]).wait()

        in_image(d, wait)

    for d in near:
        arrive(d)

    lane128 = iota((1, LANES), 1)
    for which in range(2):
        spare = iota((16, WIDE), 0) == 0
        scratch_mid[which][0][9 * 16 :, :] = jnp.where(spare, 1.0, 0.0).astype(BF16)

    def inside_mid(j):
        row = lane128 // COLS + 4 * j + 8 * (r - REACH)
        return (row >= 0) & (row < 8 * ROWS)

    def unpacked(g):
        rows = []
        for k in range(3):
            tile = None
            for j in range(4):
                at = 4 * g + j
                part = own_rows[at - 16] if 16 <= at < 24 else arrived[at].astype(F32)
                part = turned(part, COLS * (k - j))
                tile = part if tile is None else jnp.where(group == j, part, tile)
            rows.append(tile)
        return jnp.concatenate(rows, axis=0)

    steps = []
    for s in range(STEPS2):
        first, last = (0, WIDE // LANES) if s == 0 else (1, WIDE // LANES - 1)
        steps.append(
            Step(
                first, last, COLS, 12, inside_mid, wide2.at[max(s - 1, 0)],
                w1_mid.at[s], w2_mid.at[s], b2_mid.at[s], w3_mid.at[s], bias2.at[s], scratch_mid[s % 2], parts=MID_PARTS,
            )
        )
    states = [{} for _ in range(STEPS2 + 1)]
    own = (4, 5)
    loglik_terms = []

    def finish(s, j):
        step = steps[s]
        u, out = step.u[j], step.out(j)
        sigmoid, log_sigmoid = gate(out[:16])
        if j in own:
            loglik_terms.append(log_sigmoid)
        mixed = (u[8:16] + out[8:16]) * pltpu.roll(sigmoid[8:16], 4, 0)
        mixed = jnp.where(iota((8, 1), 0) < 4, u[8:16], mixed)
        rest = (u[16:24] + out[16:24]) * sigmoid[:8]
        states[s + 1][j] = jnp.concatenate([u[:8], mixed, rest], axis=0)

    for s, part, at in ORDER:
        step = steps[s]
        if part == 0:
            if s == 0:
                step.take(at, unpacked(at))
            else:
                step.mix([at], lambda j: states[s][j])
        elif part == 1:
            step.patch(at)
        elif part == 2:
            step.one(at)
        elif part == 3:
            step.two(at)
        elif part == 4:
            step.three(at)
        elif s == STEPS2 - 1 or 1 <= at < WIDE // LANES - 1:
            finish(s, at)

    final = states[STEPS2]
    for half in range(2):
        latent = final[own[half]][:16]
        loglik_terms.append(-0.5 * latent * latent)
        sent_latent[half] = latent
    loglik_sum = jnp.where(iota((16, LANES), 0) < 12, sum(loglik_terms), 0.0)

    lane, to = iota((2 * LANES, 2 * LANES), 0), iota((2 * LANES, 2 * LANES), 1)
    p, col = lane // COLS, lane % COLS
    place = (2 * (p % 2) + col % 2) * 64 + (p // 2) * 16 + col // 2
    permutation = jnp.where(place == to, 1.0, 0.0).astype(BF16)
    streams = []
    for block in range(3):
        pair = [final[2 + 2 * block], final[3 + 2 * block]]
        rest = jnp.concatenate([jnp.concatenate([x[16:24], x[8:16]], axis=0) for x in pair], axis=1)
        for _ in range(2):
            high = rest.astype(BF16)
            streams.append(high)
            rest = rest - high.astype(F32)
    apart = dot(jnp.concatenate(streams, axis=0), permutation)
    blocks = [
        apart[32 * b : 32 * b + 16] + apart[32 * b + 16 : 32 * b + 32]
        for b in range(3)
    ]
    squeezed = []
    for ij in range(4):
        half, sub = LANES * (ij // 2), 64 * (ij % 2)
        rows0, rows4, rows8 = (b[:, half : half + LANES] for b in blocks)
        left = jnp.where(lane128 < 32, turned(rows0, sub + 32), turned(rows4, sub - 32))
        left = jnp.where(lane128 < 96, left, turned(rows8, sub - 96))
        right = jnp.where(lane128 < 96, turned(rows8, sub + 32), turned(rows0, sub - 96))
        squeezed.append(jnp.concatenate([left, right], axis=1))
    state = jnp.concatenate(squeezed + [ones_block(NTOP, 16, 0)], axis=0)

    def latent_copy(k):
        to = lax.rem(c + k, CHAN)
        return pltpu.make_async_remote_copy(
            src_ref=sent_latent.at[to // 4],
            dst_ref=got_latent.at[c],
            send_sem=latent_send,
            recv_sem=latent_recv,
            device_id={"chan": to},
            device_id_type=MESH,
        )

    for k in range(1, CHAN):
        latent_copy(k).start()
    got_latent[c] = sent_latent[c // 4]

    def inside_top(j):
        row = (lane128 // 16 + 8 * j + 2) % 16
        return (row + 4 * r >= 4) & (row + 4 * r < 4 * ROWS + 4) & (row < 12)

    own_top = (lane128 >= 32) & (lane128 < 96)
    top_terms = jnp.zeros((24, LANES), F32)
    for s in range(STEPS3):
        step = Step(
            0, 2 - s, 16, 24, inside_top, wide3 if s else mix3,
            w1_top.at[s], w2_top.at[s], b2_top.at[s], w3_top.at[s], bias3.at[s], scratch_top,
            per=2 - s, wrap=None if s else 2, parts=TOP_PARTS,
        )
        step.mix(range(2 - s), lambda j: state[:, LANES * j : LANES * (j + 1)])
        step.patch(0)
        step.one(0)
        step.two(0)
        step.three(0)
        u, out = step.u[0], step.out(0)
        sigmoid, log_sigmoid = gate(out[:24])
        top_terms += log_sigmoid
        state = jnp.concatenate([u[:24], (u[24:] + out[24:]) * sigmoid], axis=0)
    z = state
    squares = z * z
    top_terms = jnp.where(own_top, top_terms - 0.5 * (squares[:24] + squares[24:]), 0.0)

    last = top_terms[:8] + top_terms[8:16] + top_terms[16:]
    last += loglik_sum[:8] + loglik_sum[8:] + base[...]
    terms[r] = jnp.sum(last, axis=0, keepdims=True) * (1.0 / DIMS)

    def term_copy(k):
        return pltpu.make_async_remote_copy(
            src_ref=terms.at[r],
            dst_ref=terms.at[r],
            send_sem=term_send,
            recv_sem=term_recv,
            device_id={"rows": (r + k) % ROWS},
            device_id_type=MESH,
        )

    for k in (4, 3, 5, 2, 6, 1, 7):
        term_copy(k).start()

    latent_top[0] = z.T[32:96].reshape(4, 16, C3)

    others = got_latent.at[pl.ds(0, CHAN - 1)]
    pltpu.make_async_copy(others, others, latent_recv).wait()
    for i in range(8):
        lined = pltpu.roll(got_latent[i], (LANES - COLS * (c % 4)) % LANES, 1)
        latent_mid[12 * i : 12 * i + 12, :] = lined[:12, :COLS]

    others = terms.at[pl.ds(0, ROWS - 1)]
    pltpu.make_async_copy(others, others, term_recv).wait()
    whole = terms[0]
    for i in range(1, ROWS):
        whole = whole + terms[i]
    loglik[...] = jnp.broadcast_to(jnp.sum(whole, axis=1, keepdims=True), (1, LANES))

    pltpu.make_async_copy(others, others, term_send).wait()
    others = got_latent.at[pl.ds(0, CHAN - 1)]
    pltpu.make_async_copy(others, others, latent_send).wait()
    for d in near:

        def left_here(d=d):
            tiles = packed_half if d else packed.at[pl.ds(0, CHAN - 1)]
            pltpu.make_async_copy(tiles, tiles, send_sem).wait()

        sends(d, left_here)


def leave(latent_mid, latent_top, loglik, latent_mid_out, latent_top_out, loglik_out, sem):
    copies = [
        pltpu.make_async_copy(src, dst, sem.at[i])
        for i, (src, dst) in enumerate(
            ((latent_mid, latent_mid_out), (latent_top, latent_top_out), (loglik, loglik_out))
        )
    ]
    for copy in copies:
        copy.start()
    for copy in copies:
        copy.wait()


def body(*given):
    given = list(given)
    given[0] = given[0].reshape(8, C2, COLS)
    given[10] = given[10].transpose(0, 1, 3, 2)
    given[21] = given[21].transpose(0, 1, 3, 2)

    def small(n, steps):
        return (
            pltpu.VMEM((steps, n), F32),
            pltpu.VMEM((steps, n), F32),
            pltpu.VMEM((steps, n, n), F32),
            pltpu.VMEM((steps, n, n), F32),
            pltpu.VMEM((steps, n), F32),
            pltpu.VMEM((steps, HID), BF16),
            pltpu.VMEM((steps, HID), F32),
            pltpu.VMEM((steps, n), F32),
        )

    def inner(taps, lanes, outs):
        return (
            pltpu.VMEM((taps, lanes), BF16),
            pltpu.VMEM((HID, lanes), BF16),
            pltpu.VMEM((HID, lanes), BF16),
            pltpu.VMEM((9 * outs, lanes), F32),
        )

    latent_mid, latent_top, loglik = pl.pallas_call(
        kernel,
        out_shape=(
            pltpu.VMEM((8 * 12, COLS), F32),
            pltpu.VMEM((1, 4, 16, C3), F32),
            pltpu.VMEM((1, LANES), F32),
        ),
        in_specs=[pl.BlockSpec(memory_space=pl.ANY)] * 23,
        out_specs=tuple(pl.BlockSpec(memory_space=pltpu.VMEM) for _ in range(3)),
        scratch_shapes=[
            pltpu.VMEM((8, C2, COLS), F32),
            pltpu.VMEM((8, 8, LANES), F32),
            pltpu.VMEM((8, 8, LANES), BF16),
            pltpu.VMEM((8 * BLOCKS, 8, LANES), BF16),
            pltpu.VMEM((8, 8, LANES), F32),
            pltpu.VMEM((STEPS2, 9, 12, HID), BF16),
            pltpu.VMEM((STEPS2, HID, HID), BF16),
            pltpu.VMEM((STEPS2, 9, C2, HID), BF16),
            pltpu.VMEM((STEPS3, 9, 24, HID), BF16),
            pltpu.VMEM((STEPS3, HID, HID), BF16),
            pltpu.VMEM((STEPS3, 9, C3, HID), BF16),
            small(C2, STEPS2),
            small(C3, STEPS3),
            pltpu.VMEM((C2, 96), BF16),
            pltpu.VMEM((STEPS2 - 1, C2 + 1, C2, LANES), F32),
            pltpu.VMEM((C3, 240), BF16),
            pltpu.VMEM((C3 + 1, C3, LANES), F32),
            pltpu.VMEM((STEPS2, C2, 1), F32),
            pltpu.VMEM((STEPS3, C3, 1), F32),
            pltpu.VMEM((KTOP, HID), F32),
            pltpu.VMEM((STEPS2, HID, KMID), BF16),
            pltpu.VMEM((STEPS2, HID, HID), BF16),
            pltpu.VMEM((STEPS2, HID, LANES), F32),
            pltpu.VMEM((STEPS2, 9 * C2, HID), BF16),
            pltpu.VMEM((STEPS3, HID, KTOP), BF16),
            pltpu.VMEM((STEPS3, HID, HID), BF16),
            pltpu.VMEM((STEPS3, HID, LANES), F32),
            pltpu.VMEM((STEPS3, 9 * C3, HID), BF16),
            pltpu.VMEM((2, 16, LANES), F32),
            pltpu.VMEM((CHAN, 16, LANES), F32),
            pltpu.VMEM((ROWS, 1, LANES), F32),
            pltpu.VMEM((8, LANES), F32),
            tuple(inner(KMID, WIDE, C2) for _ in range(2)),
            inner(KTOP, NTOP, C3),
            pltpu.SemaphoreType.DMA,
            pltpu.SemaphoreType.DMA((16,)),
            pltpu.SemaphoreType.DMA((6,)),
            pltpu.SemaphoreType.DMA,
            pltpu.SemaphoreType.DMA((BLOCKS,)),
            pltpu.SemaphoreType.DMA,
            pltpu.SemaphoreType.DMA,
            pltpu.SemaphoreType.DMA,
            pltpu.SemaphoreType.DMA,
        ],
        compiler_params=pltpu.CompilerParams(collective_id=0, has_side_effects=True, vmem_limit_bytes=60 * 2**20),
    )(*given)
    latent_mid, latent_top, loglik = pl.pallas_call(
        leave,
        out_shape=(
            jax.ShapeDtypeStruct((8 * 12, COLS), F32),
            jax.ShapeDtypeStruct((1, 4, 16, C3), F32),
            jax.ShapeDtypeStruct((1, LANES), F32),
        ),
        in_specs=[pl.BlockSpec(memory_space=pltpu.VMEM)] * 3,
        out_specs=tuple(pl.BlockSpec(memory_space=pl.ANY) for _ in range(3)),
        scratch_shapes=[pltpu.SemaphoreType.DMA((3,))],
    )(*(pltpu.with_memory_space_constraint(x, pltpu.VMEM) for x in (latent_mid, latent_top, loglik)))
    return (
        latent_mid.reshape(8, 12, 1, COLS),
        latent_top.transpose(0, 3, 1, 2),
        loglik[0, :1],
    )


def solution(mesh):
    placed = (P("batch", None, ("rows", "chan"), None),) + (P(),) * 22
    return jax.shard_map(
        body,
        mesh=mesh,
        in_specs=placed,
        out_specs=(
            P("batch", None, ("rows", "chan"), None),
            P(("batch", "chan"), None, "rows", None),
            P(("batch", "chan")),
        ),
        check_vma=False,
    )
```

```python
import math

import jax
import jax.numpy as jnp
from jax import lax
from jax.experimental import pallas as pl
from jax.experimental.pallas import tpu as pltpu
from jax.sharding import PartitionSpec as P

MESH = pl.DeviceIdType.MESH
F32 = jnp.float32
BF16 = jnp.bfloat16
LOG_TWO_PI = math.log(2.0 * math.pi)

HID = 512
ROWS = 8
CHAN = 8
C2, C3 = 24, 48
STEPS2, STEPS3 = 3, 2
COLS = 32
LANES = 128
REACH = 2
BLOCKS = 2 * REACH + 1
WIDE = BLOCKS * 8 * COLS
NARROW = WIDE - 2 * LANES
KMID = 160
KTOP = 224
NTOP = 256
DIMS = 24 * 64 * 32


def iota(shape, dim):
    return lax.broadcasted_iota(jnp.int32, shape, dim)


def dot(a, b):
    return jnp.dot(a, b, preferred_element_type=F32)


def exact_dot(a, b):
    return jnp.dot(a, b, preferred_element_type=F32, precision=lax.Precision.HIGHEST)


def column(row):
    n = row.shape[1]
    eye = iota((n, n), 0) == iota((n, n), 1)
    return jnp.sum(jnp.where(eye, row, 0.0), axis=1, keepdims=True)


def place_mid(n, dim):
    at = iota((n, n), dim)
    return jnp.where(at < 12, at, jnp.where(at < 16, at + 8, at - 4))


def mixing(shift, gain, lower, upper, diag):
    n = shift.shape[1]
    i, j = iota((n, n), 0), iota((n, n), 1)
    low = jnp.where(j < i, lower, 0.0) + jnp.where(i == j, 1.0, 0.0)
    up = jnp.where(j > i, upper, 0.0) + jnp.where(i == j, jnp.exp(diag), 0.0)
    a = exact_dot(low, up) * jnp.exp(gain)
    return a, jnp.sum(a * shift, axis=1, keepdims=True)


def stacked(a, b, width, bias_at):
    rows, n = a.shape
    if width > n:
        a = jnp.concatenate([a, jnp.zeros((rows, width - n), F32)], axis=1)
    a = jnp.where(iota((rows, width), 1) == bias_at, b, a)
    high = a.astype(BF16).astype(F32)
    low = a - high
    return jnp.concatenate([high, high, low], axis=1).astype(BF16)


def split_mix(a, v):
    high = v.astype(BF16)
    low = (v - high.astype(F32)).astype(BF16)
    return dot(a, jnp.concatenate([high, low, high], axis=0))


def roll(x, by):
    n = x.shape[1]
    by = by % n
    return x if by == 0 else pltpu.roll(x, by, 1)


def ones_block(n, height, at):
    return jnp.where(iota((height, n), 0) == at, 1.0, 0.0)


def turned(x, by):
    return pltpu.roll(x, -by % LANES, 1)


def moved(blocks, j, by, lane):
    if by == 0:
        return blocks(j, 0)
    here, beside = blocks(j, by), blocks(j + (1 if by > 0 else -1), by)
    if beside is None:
        return here
    return jnp.where(lane < LANES - by, here, beside) if by > 0 else jnp.where(lane >= -by, here, beside)


def cached(get):
    kept = {}

    def blocks(j, by):
        if (j, by) not in kept:
            x = get(j)
            kept[j, by] = x if x is None or by == 0 else turned(x, by)
        return kept[j, by]

    return blocks


def cut(rows, parts):
    each = -(-rows // parts // 8) * 8
    return [slice(at, min(at + each, rows)) for at in range(0, rows, each)]


class Step:
    def __init__(self, first, last, width, half, inside, mix, w1, w2, b2, w3, b3, scratch, per=2, wrap=None, parts=1):
        self.parts = parts
        self.first, self.last, self.width, self.half, self.per, self.wrap = first, last, width, half, per, wrap
        self.inside, self.mix_w, self.w1, self.w2, self.b2, self.w3, self.b3 = inside, mix, w1, w2, b2, w3, b3
        self.patches, self.h1, self.h2, self.z = scratch
        self.outs = w3.shape[0] // 9
        self.u, self.q = {}, {}
        self.lane = iota((1, LANES), 1)
        col = self.lane % width
        self.edge = {-1: col > 0, 1: col < width - 1}
        self.q_blocks = cached(lambda j: self.q.get(j % wrap if wrap else j))
        self.z_blocks = [
            cached(lambda j, t=t: self.z_block(t, j)) for t in range(9)
        ]

    def pair(self, t):
        return [self.first + self.per * t + i for i in range(self.per)]

    def lanes(self, t):
        return slice(self.per * LANES * t, self.per * LANES * (t + 1))

    def mix(self, blocks, state):
        if len(self.mix_w.shape) == 3:
            n = self.mix_w.shape[0] - 1
            x = [state(j) for j in blocks]
            sums = [[self.mix_w[n]] * len(x), [None] * len(x)]
            for k in range(n):
                weights = self.mix_w[k]
                for i, y in enumerate(x):
                    term, so_far = weights * y[k : k + 1, :], sums[k % 2][i]
                    sums[k % 2][i] = term if so_far is None else so_far + term
            for i, j in enumerate(blocks):
                self.take(j, sums[0][i] + sums[1][i])
            return
        u = split_mix(self.mix_w[...], jnp.concatenate([state(j) for j in blocks], axis=1))
        for i, j in enumerate(blocks):
            self.take(j, u[:, LANES * i : LANES * (i + 1)])

    def take(self, j, u):
        rows = 16 if self.half == 12 else 24
        self.u[j] = u
        self.q[j] = jnp.where(self.inside(j), u[:rows], 0.0)
        if rows == 16:
            self.q[j] = self.q[j].astype(BF16)

    def patch(self, t):
        taps = []
        for dy in (-1, 0, 1):
            for dx in (-1, 0, 1):
                parts = []
                for j in self.pair(t):
                    part = moved(self.q_blocks, j, self.width * dy + dx, self.lane)
                    parts.append(jnp.where(self.edge[dx], part, jnp.zeros_like(part)) if dx else part)
                taps.append(jnp.concatenate(parts, axis=1))
        if self.half == 12:
            for i, tap in enumerate(taps):
                self.patches[16 * i : 16 * (i + 1), self.lanes(t)] = tap
        else:
            taps.append(ones_block(self.per * LANES, 8, 0))
            self.patches[:, self.lanes(t)] = jnp.concatenate(taps, axis=0).astype(BF16)

    def one(self, t):
        patches = self.patches[:, self.lanes(t)]
        for m in cut(HID, self.parts):
            self.h1[m, self.lanes(t)] = jnp.maximum(dot(self.w1[m, :], patches), 0.0).astype(BF16)

    def two(self, t):
        h1 = self.h1[:, self.lanes(t)]
        for m in cut(HID, self.parts):
            bias = jnp.concatenate([self.b2[m, :]] * self.per, axis=1)
            self.h2[m, self.lanes(t)] = jnp.maximum(dot(self.w2[m, :], h1) + bias, 0.0).astype(BF16)

    def three(self, t):
        inside = jnp.concatenate([self.inside(j) for j in self.pair(t)], axis=1)
        h2 = self.h2[:, self.lanes(t)]
        for m in cut(9 * self.outs, self.parts):
            self.z[m, self.lanes(t)] = jnp.where(inside, dot(self.w3[m, :], h2), 0.0)

    def z_block(self, tap, j):
        if self.wrap:
            j = j % self.wrap
        if not self.first <= j < self.last:
            return None
        at = LANES * (j - self.first)
        return self.z[self.outs * tap : self.outs * (tap + 1), at : at + LANES]

    def out(self, j):
        total = self.b3[...]
        for dx in (0, -1, 1):
            side = None
            for dy in (-1, 0, 1):
                part = moved(self.z_blocks[3 * (dy + 1) + dx + 1], j, self.width * dy + dx, self.lane)
                side = part if side is None else side + part
            total = total + (jnp.where(self.edge[dx], side, 0.0) if dx else side)
        return total


def gate(g):
    small = jnp.exp(-jnp.abs(g))
    sigmoid = jnp.where(g >= 0.0, 1.0, small) / (1.0 + small)
    return sigmoid, jnp.minimum(g, 0.0) - jnp.log(1.0 + small)


def emission(windows):
    slots, done = [], {}
    for s, (first, last) in enumerate(windows):
        blocks, tiles = range(first, last), range((last - first) // 2)
        at = {}
        for j in blocks:
            at[0, j] = done[j] if s else (j - first) // 2
        end = -1
        for t in tiles:
            seen = [j for j in range(first + 2 * t - 1, first + 2 * t + 3) if j in blocks]
            at[1, t] = max(at[0, j] for j in seen) + 1
            at[2, t] = end = max(at[1, t], end + 1)
            at[3, t] = at[2, t] + LAG
            at[4, t] = at[2, t] + 2 * LAG
        for j in blocks:
            at[5, j] = max(at[4, (x - first) // 2] for x in (j - 1, j, j + 1) if x in blocks) + 1
            done[j] = at[5, j]
        slots += [(slot, s, part, x) for (part, x), slot in at.items()]
    return [(s, part, x) for _, s, part, x in sorted(slots)]


LAG = 1
MID_PARTS = 2
TOP_PARTS = 4
ORDER = emission(((0, 10), (1, 9), (1, 9)))


def kernel(
    images,
    shift_mid,
    gain_mid,
    lower_mid,
    upper_mid,
    diag_mid,
    first_mid,
    first_bias_mid,
    second_mid,
    second_bias_mid,
    third_mid,
    third_bias_mid,
    shift_top,
    gain_top,
    lower_top,
    upper_top,
    diag_top,
    first_top,
    first_bias_top,
    second_top,
    second_bias_top,
    third_top,
    third_bias_top,
    latent_mid,
    latent_top,
    loglik,
    pictures,
    packed,
    packed_half,
    arrived,
    own_rows,
    first2,
    second2,
    third2,
    first3,
    second3,
    third3,
    small2,
    small3,
    mix2,
    wide2,
    mix3,
    wide3,
    bias2,
    bias3,
    tall,
    w1_mid,
    w2_mid,
    b2_mid,
    w3_mid,
    w1_top,
    w2_top,
    b2_top,
    w3_top,
    sent_latent,
    got_latent,
    terms,
    base,
    scratch_mid,
    scratch_top,
    load_sem,
    small_sem,
    weight_sem,
    send_sem,
    recv_sem,
    latent_send,
    latent_recv,
    term_send,
    term_recv,
):
    r, c = lax.axis_index("rows"), lax.axis_index("chan")
    barrier = pltpu.get_barrier_semaphore()

    picture_load = pltpu.make_async_copy(images, pictures, load_sem)
    picture_load.start()
    given2 = (shift_mid, gain_mid, lower_mid, upper_mid, diag_mid, first_bias_mid, second_bias_mid, third_bias_mid)
    given3 = (shift_top, gain_top, lower_top, upper_top, diag_top, first_bias_top, second_bias_top, third_bias_top)
    small_loads = [
        pltpu.make_async_copy(src, dst, small_sem.at[i])
        for i, (src, dst) in enumerate(zip(given2 + given3, small2 + small3))
    ]
    for load in small_loads:
        load.start()
    given_weights = (second_mid, first_mid, third_mid, second_top, first_top, third_top)
    kept_weights = (second2, first2, third2, second3, first3, third3)
    weight_loads = [
        pltpu.make_async_copy(src, dst, weight_sem.at[i])
        for i, (src, dst) in enumerate(zip(given_weights, kept_weights))
    ]

    def in_image(d, body):
        if d == 0:
            body()
        else:
            pl.when((r + d >= 0) & (r + d < ROWS))(body)

    near = range(-REACH, REACH + 1)

    arrived[...] = jnp.zeros_like(arrived)
    def greet(d):
        for to in range(CHAN):

            def signal(to=to):
                pl.semaphore_signal(barrier, 1, device_id={"rows": r + d, "chan": to}, device_id_type=MESH)

            if d == 0:
                pl.when(c != to)(signal)
            else:
                signal()

    def greet_far(d):
        pl.semaphore_signal(barrier, 1, device_id={"rows": r + d}, device_id_type=MESH)

    for d in sorted(range(1 - ROWS, ROWS), key=lambda d: (abs(d) > REACH, -abs(d))):
        in_image(d, lambda d=d: greet(d) if abs(d) <= REACH else greet_far(d))

    picture_load.wait()
    def prepare_mix(s):
        shift, gain, lower, upper, diag, _, second_b, third_b = small2
        a, b = mixing(shift[s : s + 1], gain[s : s + 1], lower[s], upper[s], diag[s : s + 1])
        to_rows = jnp.where(place_mid(C2, 0) == iota((C2, C2), 1), 1.0, 0.0)
        a, b = exact_dot(to_rows, a), exact_dot(to_rows, b)
        if s:
            to_columns = jnp.where(place_mid(C2, 1) == iota((C2, C2), 0), 1.0, 0.0)
            a = exact_dot(a, to_columns)
        if s == 0:
            mix2[...] = stacked(a, b, 32, C2)
        else:
            for k in range(C2):
                wide2[s - 1, k] = jnp.broadcast_to(a[:, k : k + 1], (C2, LANES))
            wide2[s - 1, C2] = jnp.broadcast_to(b, (C2, LANES))
        extra = third_b[s : s + 1] + jnp.where(iota((1, C2), 1) < C2 // 2, 2.0, 0.0)
        bias2[s] = jnp.sum(to_rows * extra, axis=1, keepdims=True)

    def prepare_small():
        for s in range(STEPS2):
            if s:
                prepare_mix(s)
            b2_mid[s] = jnp.broadcast_to(small2[6][s : s + 1], (LANES, HID)).T
        shift, gain, lower, upper, diag, _, second_b, third_b = small3
        for s in range(STEPS3):
            a, b = mixing(shift[s : s + 1], gain[s : s + 1], lower[s], upper[s], diag[s : s + 1])
            if s == 0:
                n, k = iota((C3, 64), 0), iota((C3, 64), 1)
                row = n // 4
                at = (n % 4) * 16 + jnp.where(row < 8, row, row + 4)
                a = exact_dot(a, jnp.where(at == k, 1.0, 0.0))
                mix3[...] = stacked(a, b, 80, 64)
            else:
                for k in range(C3):
                    wide3[k] = jnp.broadcast_to(a[:, k : k + 1], (C3, LANES))
                wide3[C3] = jnp.broadcast_to(b, (C3, LANES))
            extra = third_b[s : s + 1] + jnp.where(iota((1, C3), 1) < C3 // 2, 2.0, 0.0)
            bias3[s] = column(extra)
            b2_top[s] = jnp.broadcast_to(second_b[s : s + 1], (LANES, HID)).T

        logdets = 256.0 * (jnp.sum(small2[1][...]) + jnp.sum(small2[4][...]))
        logdets += 64.0 * (jnp.sum(small3[1][...]) + jnp.sum(small3[4][...]))
        logdets -= 0.5 * LOG_TWO_PI * (12 * 256 + 48 * 64)
        corner = (iota((8, LANES), 0) == 0) & (iota((8, LANES), 1) == 0)
        base[...] = jnp.where(corner, logdets, 0.0)

    def prepare_mid(s):
        if s == 0:
            for load in weight_loads[:3]:
                load.wait()
        w2_mid[s] = second2[s].T
        tall[...] = jnp.zeros_like(tall)
        for t in range(9):
            tall[16 * t : 16 * t + 12, :] = first2[s, t].astype(F32)
        tall[144:145, :] = small2[5][s : s + 1].astype(F32)
        w1_mid[s] = tall[:KMID, :].T.astype(BF16)
        to_rows = jnp.where(place_mid(C2, 0) == iota((C2, C2), 1), 1.0, 0.0).astype(BF16)
        for t in range(9):
            w3_mid[s, C2 * t : C2 * (t + 1), :] = dot(to_rows, third2[s, t]).astype(BF16)

    def prepare_top(s):
        if s == 0:
            for load in weight_loads[3:]:
                load.wait()
        w2_top[s] = second3[s].T
        for t in range(9):
            tall[24 * t : 24 * (t + 1), :] = first3[s, t].astype(F32)
            w3_top[s, C3 * t : C3 * (t + 1), :] = third3[s, t]
        tall[216:217, :] = small3[5][s : s + 1].astype(F32)
        tall[217:, :] = jnp.zeros((KTOP - 217, HID), F32)
        w1_top[s] = tall[...].T.astype(BF16)

    for load in small_loads:
        load.wait()
    for load in weight_loads:
        load.start()
    prepare_mix(0)
    group = iota((8, LANES), 1) // COLS
    pictures_in = []
    for half in range(2):
        rows = []
        for k in range(3):
            tile = None
            for j in range(4):
                part = pictures[4 * half + j, 8 * k : 8 * k + 8, :]
                part = jnp.concatenate([part, jnp.zeros((8, LANES - COLS), F32)], axis=1)
                part = turned(part, -COLS * j)
                tile = part if tile is None else jnp.where(group == j, part, tile)
            rows.append(tile)
        pictures_in.append(jnp.concatenate(rows + [ones_block(LANES, 8, 0)], axis=0))
    mixed_in = split_mix(mix2[...], jnp.concatenate(pictures_in, axis=1))

    for i in range(8):
        tile = jnp.zeros((8, LANES), F32)
        for k in range(3):
            part = mixed_in[8 * k : 8 * k + 8, LANES * (i // 4) : LANES * (i // 4 + 1)]
            tile = jnp.where(group == k, turned(part, COLS * (i % 4 - k)), tile)
        tile = pltpu.roll(tile, COLS * (c % 4), 1)
        packed[i] = tile
        packed_half[i] = tile.astype(BF16)

    for edge in range(REACH + 1):
        blocks = REACH + 1 + edge

        def meet(blocks=blocks):
            pl.semaphore_wait(barrier, CHAN * blocks - 1 + ROWS - blocks)

        if edge < REACH:
            pl.when((r == edge) | (r == ROWS - 1 - edge))(meet)
        else:
            pl.when((r >= edge) & (r <= ROWS - 1 - edge))(meet)

    def row_copy(d, k):
        to = lax.rem(c + k, CHAN)
        return pltpu.make_async_remote_copy(
            src_ref=packed_half.at[to] if d else packed.at[to],
            dst_ref=arrived.at[8 * (REACH - d) + c] if d else own_rows.at[c],
            send_sem=send_sem,
            recv_sem=recv_sem.at[REACH - d],
            device_id={"rows": r + d, "chan": to},
            device_id_type=MESH,
        )

    def sends(d, body):
        if d == REACH:
            pl.when((r + d < ROWS) & (c >= 2))(body)
        elif d == -REACH:
            pl.when((r + d >= 0) & (c < CHAN - 2))(body)
        else:
            in_image(d, body)

    for d in sorted(near, key=lambda d: -abs(d)):

        def send(d=d):
            for k in (4, 3, 5, 2, 6, 1, 7) + (() if d == 0 else (0,)):
                row_copy(d, k).start()

        sends(d, send)
    own_rows[c] = packed[c]

    prepare_small()
    for s in range(STEPS2):
        prepare_mid(s)
    for s in range(STEPS3):
        prepare_top(s)

    def arrive(d):
        first, last = 8 * (d + REACH), 8 * (d + REACH) + 8
        if d == -REACH:
            first += 2
        elif d == REACH:
            last -= 2
        tiles = arrived.at[pl.ds(first, last - first)] if d else own_rows.at[pl.ds(0, CHAN - 1)]

        def wait():
            pltpu.make_async_copy(tiles, tiles, recv_sem.at[d + REACH]).wait()

        in_image(d, wait)

    for d in near:
        arrive(d)

    lane128 = iota((1, LANES), 1)
    for which in range(2):
        spare = iota((16, WIDE), 0) == 0
        scratch_mid[which][0][9 * 16 :, :] = jnp.where(spare, 1.0, 0.0).astype(BF16)

    def inside_mid(j):
        row = lane128 // COLS + 4 * j + 8 * (r - REACH)
        return (row >= 0) & (row < 8 * ROWS)

    def unpacked(g):
        rows = []
        for k in range(3):
            tile = None
            for j in range(4):
                at = 4 * g + j
                part = own_rows[at - 16] if 16 <= at < 24 else arrived[at].astype(F32)
                tile = part if tile is None else jnp.where(group == (j + k) % 4, part, tile)
            rows.append(turned(tile, COLS * k) if k else tile)
        return jnp.concatenate(rows, axis=0)

    steps = []
    for s in range(STEPS2):
        first, last = (0, WIDE // LANES) if s == 0 else (1, WIDE // LANES - 1)
        steps.append(
            Step(
                first, last, COLS, 12, inside_mid, wide2.at[max(s - 1, 0)],
                w1_mid.at[s], w2_mid.at[s], b2_mid.at[s], w3_mid.at[s], bias2.at[s], scratch_mid[s % 2], parts=MID_PARTS,
            )
        )
    states = [{} for _ in range(STEPS2 + 1)]
    own = (4, 5)
    loglik_terms = []

    def finish(s, j):
        step = steps[s]
        u, out = step.u[j], step.out(j)
        sigmoid, log_sigmoid = gate(out[:16])
        if j in own:
            loglik_terms.append(log_sigmoid)
        mixed = (u[8:16] + out[8:16]) * pltpu.roll(sigmoid[8:16], 4, 0)
        mixed = jnp.where(iota((8, 1), 0) < 4, u[8:16], mixed)
        rest = (u[16:24] + out[16:24]) * sigmoid[:8]
        states[s + 1][j] = jnp.concatenate([u[:8], mixed, rest], axis=0)

    for s, part, at in ORDER:
        step = steps[s]
        if part == 0:
            if s == 0:
                step.take(at, unpacked(at))
            else:
                step.mix([at], lambda j: states[s][j])
        elif part == 1:
            step.patch(at)
        elif part == 2:
            step.one(at)
        elif part == 3:
            step.two(at)
        elif part == 4:
            step.three(at)
        elif s == STEPS2 - 1 or 1 <= at < WIDE // LANES - 1:
            finish(s, at)

    final = states[STEPS2]
    for half in range(2):
        latent = final[own[half]][:16]
        loglik_terms.append(-0.5 * latent * latent)
        sent_latent[half] = latent
    loglik_sum = jnp.where(iota((16, LANES), 0) < 12, sum(loglik_terms), 0.0)

    lane, to = iota((2 * LANES, 2 * LANES), 0), iota((2 * LANES, 2 * LANES), 1)
    p, col = lane // COLS, lane % COLS
    place = (2 * (p % 2) + col % 2) * 64 + (p // 2) * 16 + col // 2
    permutation = jnp.where(place == to, 1.0, 0.0).astype(BF16)
    streams = []
    for block in range(3):
        pair = [final[2 + 2 * block], final[3 + 2 * block]]
        rest = jnp.concatenate([jnp.concatenate([x[16:24], x[8:16]], axis=0) for x in pair], axis=1)
        for _ in range(2):
            high = rest.astype(BF16)
            streams.append(high)
            rest = rest - high.astype(F32)
    apart = dot(jnp.concatenate(streams, axis=0), permutation)
    blocks = [
        apart[32 * b : 32 * b + 16] + apart[32 * b + 16 : 32 * b + 32]
        for b in range(3)
    ]
    squeezed = []
    for ij in range(4):
        half, sub = LANES * (ij // 2), 64 * (ij % 2)
        rows0, rows4, rows8 = (b[:, half : half + LANES] for b in blocks)
        left = jnp.where(lane128 < 32, turned(rows0, sub + 32), turned(rows4, sub - 32))
        left = jnp.where(lane128 < 96, left, turned(rows8, sub - 96))
        right = jnp.where(lane128 < 96, turned(rows8, sub + 32), turned(rows0, sub - 96))
        squeezed.append(jnp.concatenate([left, right], axis=1))
    state = jnp.concatenate(squeezed + [ones_block(NTOP, 16, 0)], axis=0)

    def latent_copy(k):
        to = lax.rem(c + k, CHAN)
        return pltpu.make_async_remote_copy(
            src_ref=sent_latent.at[to // 4],
            dst_ref=got_latent.at[c],
            send_sem=latent_send,
            recv_sem=latent_recv,
            device_id={"chan": to},
            device_id_type=MESH,
        )

    for k in range(1, CHAN):
        latent_copy(k).start()
    got_latent[c] = sent_latent[c // 4]

    def inside_top(j):
        row = (lane128 // 16 + 8 * j + 2) % 16
        return (row + 4 * r >= 4) & (row + 4 * r < 4 * ROWS + 4) & (row < 12)

    own_top = (lane128 >= 32) & (lane128 < 96)
    top_terms = jnp.zeros((24, LANES), F32)
    for s in range(STEPS3):
        step = Step(
            0, 2 - s, 16, 24, inside_top, wide3 if s else mix3,
            w1_top.at[s], w2_top.at[s], b2_top.at[s], w3_top.at[s], bias3.at[s], scratch_top,
            per=2 - s, wrap=None if s else 2, parts=TOP_PARTS,
        )
        step.mix(range(2 - s), lambda j: state[:, LANES * j : LANES * (j + 1)])
        step.patch(0)
        step.one(0)
        step.two(0)
        step.three(0)
        u, out = step.u[0], step.out(0)
        sigmoid, log_sigmoid = gate(out[:24])
        top_terms += log_sigmoid
        state = jnp.concatenate([u[:24], (u[24:] + out[24:]) * sigmoid], axis=0)
    z = state
    squares = z * z
    top_terms = jnp.where(own_top, top_terms - 0.5 * (squares[:24] + squares[24:]), 0.0)

    last = top_terms[:8] + top_terms[8:16] + top_terms[16:]
    last += loglik_sum[:8] + loglik_sum[8:] + base[...]
    terms[r] = jnp.sum(last, axis=0, keepdims=True) * (1.0 / DIMS)

    def term_copy(k):
        return pltpu.make_async_remote_copy(
            src_ref=terms.at[r],
            dst_ref=terms.at[r],
            send_sem=term_send,
            recv_sem=term_recv,
            device_id={"rows": (r + k) % ROWS},
            device_id_type=MESH,
        )

    for k in (4, 3, 5, 2, 6, 1, 7):
        term_copy(k).start()

    latent_top[0] = z.T[32:96].reshape(4, 16, C3)

    others = got_latent.at[pl.ds(0, CHAN - 1)]
    pltpu.make_async_copy(others, others, latent_recv).wait()
    for i in range(8):
        lined = pltpu.roll(got_latent[i], (LANES - COLS * (c % 4)) % LANES, 1)
        latent_mid[12 * i : 12 * i + 12, :] = lined[:12, :COLS]

    others = terms.at[pl.ds(0, ROWS - 1)]
    pltpu.make_async_copy(others, others, term_recv).wait()
    whole = terms[0]
    for i in range(1, ROWS):
        whole = whole + terms[i]
    loglik[...] = jnp.broadcast_to(jnp.sum(whole, axis=1, keepdims=True), (1, LANES))

    pltpu.make_async_copy(others, others, term_send).wait()
    others = got_latent.at[pl.ds(0, CHAN - 1)]
    pltpu.make_async_copy(others, others, latent_send).wait()
    for d in near:

        def left_here(d=d):
            tiles = packed_half if d else packed.at[pl.ds(0, CHAN - 1)]
            pltpu.make_async_copy(tiles, tiles, send_sem).wait()

        sends(d, left_here)


def leave(latent_mid, latent_top, loglik, latent_mid_out, latent_top_out, loglik_out, sem):
    copies = [
        pltpu.make_async_copy(src, dst, sem.at[i])
        for i, (src, dst) in enumerate(
            ((latent_mid, latent_mid_out), (latent_top, latent_top_out), (loglik, loglik_out))
        )
    ]
    for copy in copies:
        copy.start()
    for copy in copies:
        copy.wait()


def body(*given):
    given = list(given)
    given[0] = given[0].reshape(8, C2, COLS)
    given[10] = given[10].transpose(0, 1, 3, 2)
    given[21] = given[21].transpose(0, 1, 3, 2)

    def small(n, steps):
        return (
            pltpu.VMEM((steps, n), F32),
            pltpu.VMEM((steps, n), F32),
            pltpu.VMEM((steps, n, n), F32),
            pltpu.VMEM((steps, n, n), F32),
            pltpu.VMEM((steps, n), F32),
            pltpu.VMEM((steps, HID), BF16),
            pltpu.VMEM((steps, HID), F32),
            pltpu.VMEM((steps, n), F32),
        )

    def inner(taps, lanes, outs):
        return (
            pltpu.VMEM((taps, lanes), BF16),
            pltpu.VMEM((HID, lanes), BF16),
            pltpu.VMEM((HID, lanes), BF16),
            pltpu.VMEM((9 * outs, lanes), F32),
        )

    latent_mid, latent_top, loglik = pl.pallas_call(
        kernel,
        out_shape=(
            pltpu.VMEM((8 * 12, COLS), F32),
            pltpu.VMEM((1, 4, 16, C3), F32),
            pltpu.VMEM((1, LANES), F32),
        ),
        in_specs=[pl.BlockSpec(memory_space=pl.ANY)] * 23,
        out_specs=tuple(pl.BlockSpec(memory_space=pltpu.VMEM) for _ in range(3)),
        scratch_shapes=[
            pltpu.VMEM((8, C2, COLS), F32),
            pltpu.VMEM((8, 8, LANES), F32),
            pltpu.VMEM((8, 8, LANES), BF16),
            pltpu.VMEM((8 * BLOCKS, 8, LANES), BF16),
            pltpu.VMEM((8, 8, LANES), F32),
            pltpu.VMEM((STEPS2, 9, 12, HID), BF16),
            pltpu.VMEM((STEPS2, HID, HID), BF16),
            pltpu.VMEM((STEPS2, 9, C2, HID), BF16),
            pltpu.VMEM((STEPS3, 9, 24, HID), BF16),
            pltpu.VMEM((STEPS3, HID, HID), BF16),
            pltpu.VMEM((STEPS3, 9, C3, HID), BF16),
            small(C2, STEPS2),
            small(C3, STEPS3),
            pltpu.VMEM((C2, 96), BF16),
            pltpu.VMEM((STEPS2 - 1, C2 + 1, C2, LANES), F32),
            pltpu.VMEM((C3, 240), BF16),
            pltpu.VMEM((C3 + 1, C3, LANES), F32),
            pltpu.VMEM((STEPS2, C2, 1), F32),
            pltpu.VMEM((STEPS3, C3, 1), F32),
            pltpu.VMEM((KTOP, HID), F32),
            pltpu.VMEM((STEPS2, HID, KMID), BF16),
            pltpu.VMEM((STEPS2, HID, HID), BF16),
            pltpu.VMEM((STEPS2, HID, LANES), F32),
            pltpu.VMEM((STEPS2, 9 * C2, HID), BF16),
            pltpu.VMEM((STEPS3, HID, KTOP), BF16),
            pltpu.VMEM((STEPS3, HID, HID), BF16),
            pltpu.VMEM((STEPS3, HID, LANES), F32),
            pltpu.VMEM((STEPS3, 9 * C3, HID), BF16),
            pltpu.VMEM((2, 16, LANES), F32),
            pltpu.VMEM((CHAN, 16, LANES), F32),
            pltpu.VMEM((ROWS, 1, LANES), F32),
            pltpu.VMEM((8, LANES), F32),
            tuple(inner(KMID, WIDE, C2) for _ in range(2)),
            inner(KTOP, NTOP, C3),
            pltpu.SemaphoreType.DMA,
            pltpu.SemaphoreType.DMA((16,)),
            pltpu.SemaphoreType.DMA((6,)),
            pltpu.SemaphoreType.DMA,
            pltpu.SemaphoreType.DMA((BLOCKS,)),
            pltpu.SemaphoreType.DMA,
            pltpu.SemaphoreType.DMA,
            pltpu.SemaphoreType.DMA,
            pltpu.SemaphoreType.DMA,
        ],
        compiler_params=pltpu.CompilerParams(collective_id=0, has_side_effects=True, vmem_limit_bytes=60 * 2**20),
    )(*given)
    latent_mid, latent_top, loglik = pl.pallas_call(
        leave,
        out_shape=(
            jax.ShapeDtypeStruct((8 * 12, COLS), F32),
            jax.ShapeDtypeStruct((1, 4, 16, C3), F32),
            jax.ShapeDtypeStruct((1, LANES), F32),
        ),
        in_specs=[pl.BlockSpec(memory_space=pltpu.VMEM)] * 3,
        out_specs=tuple(pl.BlockSpec(memory_space=pl.ANY) for _ in range(3)),
        scratch_shapes=[pltpu.SemaphoreType.DMA((3,))],
    )(*(pltpu.with_memory_space_constraint(x, pltpu.VMEM) for x in (latent_mid, latent_top, loglik)))
    return (
        latent_mid.reshape(8, 12, 1, COLS),
        latent_top.transpose(0, 3, 1, 2),
        loglik[0, :1],
    )


def solution(mesh):
    placed = (P("batch", None, ("rows", "chan"), None),) + (P(),) * 22
    return jax.shard_map(
        body,
        mesh=mesh,
        in_specs=placed,
        out_specs=(
            P("batch", None, ("rows", "chan"), None),
            P(("batch", "chan"), None, "rows", None),
            P(("batch", "chan")),
        ),
        check_vma=False,
    )
```
